32 devices in a mesh: tm: 4 (over y, x), users: 8 (over z, core).
Axes of the slice: x: 2, y: 2, z: 4, core: 2. Of those that a mesh axis runs over, the one named last changes fastest.
Arguments:
- features: float32 [131072, 128], P(('tm', 'users')), may hold values from -6 to 6
- home: int32 [131072, 1], P(('tm', 'users')), may hold values from 0 to 7; in each aligned block of 4096 rows (0 to 4095, 4096 to 8191, ...) at most 1024 rows name the same one
- account: int32 [131072], P(('tm', 'users')), may hold values from 0 to 127
- flags: int32 [131072], P(('tm', 'users')), may hold values 0 or 1
Outputs:
- session_mean: float32 [131072, 128], P(('tm', 'users'))
The draws below stay inside these ranges and needn't reach their ends.
Inputs may be any that keep to these rules, and one draw needn't show every extreme that they name: `home`: the 4096 events of one device name one owner at most 1024 times, a bound that some block reaches.
All inputs are finite; a program needn't handle non-finite values. No bound on the sum of `flags` on one device may be relied on, other than what follows from the above.
Results may differ from the reference program's by a relative error of at most 0.00007.
Values sent between devices are 32-bit elements; how exact they have to be, the bound alone decides.
No kernel may reach another device: no remote copies, remote signals or barrier semaphores. Data moves between devices by JAX's collectives and lax.ppermute only.
A program may use at most 64 MiB of HBM per device.

```python
import math
import jax
import jax.numpy as jnp
import numpy as np
from jax import lax

F = 128
EV_DEV = 4096
ACCOUNTS = 128
CAP = 1024
EVENTS = 131072
N_USERS = 8


def set_ends(array, key, least, largest):
    spot = [jax.random.randint(jax.random.fold_in(key, axis), (), 0, length) for axis, length in enumerate(array.shape)]
    longest = array.shape.index(max(array.shape))
    beside = spot[:longest] + [(spot[longest] + 1) % array.shape[longest]] + spot[longest + 1:]
    return array.at[tuple(spot)].set(least).at[tuple(beside)].set(largest)


def levels(key, dims, shards, low, high):
    def one(position, shards_of):
        heights = jax.random.uniform(jax.random.fold_in(jax.random.fold_in(key, 6), position), (shards_of,), jnp.float32, low / len(shards), high / len(shards))
        return jnp.repeat(jnp.exp(heights), dims[position] // shards_of).reshape((-1,) + (1,) * (len(dims) - position - 1))

    gain = one(*shards[0])
    for cut in shards[1:]:
        gain = gain * one(*cut)
    return gain


def routed_block(key, own, number, rows, number_of, top, most, lean):
    sequence = jax.random.permutation(key, number_of)
    heavy_load, usual = load_shares(number_of, rows * top, most, lean, True), load_shares(number_of, rows * top, most, lean, False)
    places = jnp.arange(number_of)

    def named(lengths, turn):
        used = int((lengths > 0).sum())
        fixed = max(1, used // 4)
        shifted = fixed + (places - fixed + turn * (used - fixed)) % max(1, number_of - fixed)
        return jnp.zeros((number_of,), jnp.int32).at[sequence[jnp.where(places < fixed, places, shifted)]].set(jnp.asarray(lengths, jnp.int32))

    lengths = jnp.where(number % 4 == 0, named(heavy_load, number // 4), named(usual, number - number // 4 - 1))
    mixed = jax.random.permutation(jax.random.fold_in(own, 3), number_of)
    source_of, receiver = mixed[0:number_of // 2 * 2:2], mixed[1:number_of // 2 * 2:2]
    margin = jnp.minimum(lengths[source_of] - 1, most - lengths[receiver]) // 2
    margin = jnp.where((source_of == sequence[0]) | (receiver == sequence[0]) | (lengths[receiver] == 0), 0, jnp.maximum(margin, 0))
    shifted = jax.random.randint(jax.random.fold_in(own, 4), (number_of // 2,), 0, 1 << 20) % (margin + 1)
    lengths = lengths.at[source_of].add(-shifted).at[receiver].add(shifted)
    labels = jnp.searchsorted(jnp.cumsum(lengths), jnp.arange(rows * top), side="right").astype(jnp.int32)
    table = labels.reshape(top, rows).T
    table = table[jax.random.permutation(jax.random.fold_in(own, 1), rows)]
    turn = jax.random.randint(jax.random.fold_in(own, 2), (rows, 1), 0, top)
    return jnp.take_along_axis(table, (jnp.arange(top)[None, :] + turn) % top, axis=1)


def load_shares(count, total, limit, slope, full):
    weights = [(1 << 20) // math.isqrt(grade ** slope) + 1 for grade in range(1, count + 1)]
    largest = limit if full else min(limit, max(-(-total // count), total * weights[0] // sum(weights)))
    least = 1 if total - largest >= count - 1 else 0
    given, spare = [largest] + [least] * (count - 1), total - largest - least * (count - 1)
    while spare > 0:
        candidates = [i for i in range(1, count) if given[i] < largest] or [i for i in range(1, count) if given[i] < limit]
        mass, remaining = sum([weights[i] for i in candidates]), spare
        for i in candidates:
            extra = min(limit - given[i], max(1, remaining * weights[i] // mass), spare)
            given[i] = given[i] + extra
            spare = spare - extra
    return np.array(given)


def gaussian(stream_key, extent, deviation, bound, shards=(), dtype=jnp.bfloat16):
    gain = levels(stream_key, extent, shards, -0.22, 0.18) if shards else 1.0
    drawn = jax.random.normal(stream_key, extent, jnp.float32) * deviation * gain
    return jnp.minimum(jnp.maximum(drawn, -bound), bound).astype(dtype)


def setup_inputs(seed: int = 0) -> dict:
    key_list = jax.random.split(jax.random.key(seed), 5)
    features = gaussian(key_list[0], (EVENTS, F), 1.0, 6.0, ((0, 32),), jnp.float32)
    home_keys = jax.random.split(jax.random.fold_in(key_list[1], 1), EVENTS // EV_DEV)
    home_turns = jax.random.permutation(jax.random.fold_in(key_list[1], 3), EVENTS // EV_DEV)
    home = jax.vmap(lambda own, number: routed_block(jax.random.fold_in(key_list[1], 2), own, number, EV_DEV, N_USERS, 1, CAP, 2))(home_keys, home_turns).reshape((EVENTS, 1))
    account = set_ends(jax.random.randint(key_list[2], (EVENTS,), 0, ACCOUNTS), jax.random.fold_in(key_list[2], 1), 0, ACCOUNTS - 1).astype(jnp.int32)
    flags = set_ends((jax.random.randint(key_list[3], (EVENTS,), 0, 64) < 1).astype(jnp.int32), jax.random.fold_in(key_list[3], 1), 0, 1)
    return dict(features=features, home=home, account=account, flags=flags)


def combine_runs(earlier, later):
    carry_on = 1.0 - later[2]
    return (later[0] + carry_on[..., None] * earlier[0], later[1] + carry_on * earlier[1], jnp.maximum(earlier[2], later[2]))


def reference(features, home, account, flags):
    user = home[:, 0].astype(jnp.int32) * ACCOUNTS + account.astype(jnp.int32)
    order = jnp.argsort(user, stable=True)
    user_sorted = user[order]
    flag_sorted = flags[order].astype(jnp.int32)
    values = features[order]
    changed = jnp.concatenate([jnp.ones((1,), jnp.int32), (user_sorted[1:] != user_sorted[:-1]).astype(jnp.int32)])
    starts = jnp.maximum(changed, flag_sorted).astype(jnp.float32)
    singles = jnp.ones(starts.shape, jnp.float32)
    sums, counts, marks = lax.associative_scan(combine_runs, (values, singles, starts))
    means = sums / counts[:, None]
    return jnp.zeros_like(features).at[order].set(means)
```

```python
import functools

import jax
import jax.numpy as jnp
from jax import lax
from jax.experimental import pallas as pl
from jax.experimental.pallas import tpu as pltpu
from jax.sharding import PartitionSpec as P

ACCOUNTS = 128
LANES = 128
EXTRA = 8
HALVINGS = 2
AXES = ("tm", "users")
F32, BF16, I32 = jnp.float32, jnp.bfloat16, jnp.int32


def split_two(x):
    high = x.astype(BF16)
    return high, (x - high.astype(F32)).astype(BF16)


def sublane_ids():
    return lax.broadcasted_iota(I32, (ACCOUNTS, LANES), 0).astype(F32)


def row_positions(tiles):
    shape = (tiles, LANES)
    return lax.broadcasted_iota(I32, shape, 0) * LANES + lax.broadcasted_iota(I32, shape, 1)


def one_hot_tile(key_row, ids):
    return key_row == ids


def last_flag_row(kept, ids):
    tiles = kept.shape[0]
    latest = jnp.full((ACCOUNTS, LANES), -1.0, F32)
    for tile in range(tiles):
        latest = jnp.where(kept[tile : tile + 1] == ids, float(tile), latest)
    lane = lax.broadcasted_iota(I32, (ACCOUNTS, LANES), 1).astype(F32)
    place = jnp.where(latest >= 0.0, latest * LANES + lane, -1.0)
    return jnp.max(place.T, axis=0, keepdims=True)


def closing_kernel(flip_ref, home_ref, account_ref, flag_ref, x_ref, out_ref, parts_ref, last_ref):
    tiles = home_ref.shape[0]
    owners, rows = out_ref.shape[0], out_ref.shape[1]
    features = x_ref.shape[1]
    events = x_ref.shape[0]
    chunk = min(512, events)
    per_chunk = chunk // LANES
    group = 2 if owners % 2 == 0 else 1
    flip = flip_ref[0]
    ids = sublane_ids()
    home = home_ref[...]
    account = account_ref[...]
    flag = flag_ref[...]
    account_f = account.astype(F32)

    high, low = split_two(x_ref[...])
    parts_ref[:, 0:features] = high
    parts_ref[:, features : 2 * features] = low

    def find_last(owner, carry):
        kept = jnp.where((home == owner) & (flag == 1), account_f, -1.0)
        last_ref[pl.ds(owner, 1), :] = last_flag_row(kept, ids)
        return carry

    lax.fori_loop(0, owners, find_last, 0, unroll=min(owners, 4))

    def look_up(owner, least):
        row = jnp.broadcast_to(last_ref[pl.ds(owner, 1), :], (tiles, LANES))
        found = jnp.take_along_axis(row, account, axis=1)
        return jnp.where(home == owner, found, least)

    least = lax.fori_loop(
        0, owners, look_up, jnp.full((tiles, LANES), -1.0, F32), unroll=min(owners, 8)
    )
    live = row_positions(tiles).astype(F32) >= least
    weight = jnp.where(flag == 1, 8193.0, 1.0)

    def one_group(number, carry):
        kept = [
            jnp.where(live & (home == number * group + i), account_f, -1.0) for i in range(group)
        ]
        total = jnp.zeros((group * ACCOUNTS, 2 * features), F32)
        counts = [jnp.zeros((ACCOUNTS, LANES), F32) for i in range(group)]
        for first in range(0, events, chunk):
            blocks = []
            for i in range(group):
                pieces = []
                for tile in range(first // LANES, first // LANES + per_chunk):
                    mask = kept[i][tile : tile + 1] == ids
                    counts[i] = counts[i] + jnp.where(mask, weight[tile : tile + 1], 0.0)
                    pieces.append(jnp.where(mask, 1.0, 0.0).astype(BF16))
                blocks.append(jnp.concatenate(pieces, axis=1))
            total = total + jnp.dot(
                jnp.concatenate(blocks, axis=0),
                parts_ref[first : first + chunk, :],
                preferred_element_type=F32,
            )
        sums = total[:, 0:features] + total[:, features : 2 * features]
        for i in range(group):
            place = jnp.bitwise_xor(number * group + i, flip)
            mine = sums[i * ACCOUNTS : (i + 1) * ACCOUNTS]
            out_ref[place, 0:features, :] = mine.T
            tally = jnp.sum(counts[i].T, axis=0, keepdims=True)
            marked = jnp.where(tally >= 8192.0, 1.0, 0.0)
            spot = lax.broadcasted_iota(I32, (rows - features, LANES), 0)
            out_ref[place, features:rows, :] = jnp.where(
                spot == 0, tally - 8192.0 * marked, jnp.where(spot == 1, marked, 0.0)
            )
        return carry

    lax.fori_loop(0, owners // group, one_group, 0)


def local_kernel(
    home_ref, account_ref, flag_ref, x_ref, out_ref, key_ref, parts_ref, column_ref, start_ref, sid_ref
):
    tiles = home_ref.shape[0]
    events, features = x_ref.shape
    rows = parts_ref.shape[0]
    chunk = min(512, events)
    per_chunk = chunk // LANES
    home = home_ref[...]
    account = account_ref[...]
    flag = flag_ref[...]
    user = home * ACCOUNTS + account
    user_f = user.astype(F32)
    sid_ref[...] = user_f
    flagged = jnp.where(flag == 1, user_f, -1.0)
    row_id = lax.broadcasted_iota(I32, (LANES, LANES), 0)
    column_id = lax.broadcasted_iota(I32, (LANES, LANES), 1)
    reaches = row_id <= column_id
    spot = row_id.astype(F32)

    for tile in range(tiles):
        span = slice(tile * LANES, (tile + 1) * LANES)
        turned = x_ref[span, :].T
        high, low = split_two(turned)
        parts_ref[0:features, span] = high
        parts_ref[features : 2 * features, span] = low
        column_ref[span, :] = jnp.broadcast_to(flagged[tile : tile + 1], (LANES, LANES)).T
    extra = lax.broadcasted_iota(I32, (rows - 2 * features, events), 0)
    parts_ref[2 * features : rows, :] = jnp.where(extra == 0, 1.0, 0.0).astype(BF16)

    def find_start(tile, carry):
        mine = sid_ref[pl.ds(tile, 1), :]

        def earlier(other, latest):
            column = column_ref[pl.ds(other * LANES, LANES), :]
            place = spot + (other * LANES).astype(F32)
            return jnp.where(column == mine, place, latest)

        latest = lax.fori_loop(0, tile, earlier, jnp.full((LANES, LANES), -1.0, F32))
        column = column_ref[pl.ds(tile * LANES, LANES), :]
        place = spot + (tile * LANES).astype(F32)
        latest = jnp.where((column == mine) & reaches, place, latest)
        start_ref[pl.ds(tile, 1), :] = jnp.max(latest, axis=0, keepdims=True)
        return carry

    lax.fori_loop(0, tiles, find_start, 0)
    start = start_ref[...]
    key_ref[...] = jnp.where(start < 0.0, user, -1)
    sid = jnp.where(start < 0.0, user_f + float(events), start)
    sid_ref[...] = sid
    for tile in range(tiles):
        span = slice(tile * LANES, (tile + 1) * LANES)
        column_ref[span, :] = jnp.broadcast_to(sid[tile : tile + 1], (LANES, LANES)).T

    def mask_block(first_c, first_r, diagonal):
        pieces = []
        for a in range(per_chunk):
            column = column_ref[pl.ds(first_c + a * LANES, LANES), :]
            line = []
            for b in range(per_chunk):
                if diagonal and a > b:
                    line.append(jnp.zeros((LANES, LANES), BF16))
                    continue
                mine = sid_ref[pl.ds(first_r // LANES + b, 1), :]
                mask = column == mine
                if diagonal and a == b:
                    mask = mask & reaches
                line.append(jnp.where(mask, 1.0, 0.0).astype(BF16))
            pieces.append(jnp.concatenate(line, axis=1))
        return jnp.concatenate(pieces, axis=0)

    for number in range(events // chunk):
        first_r = number * chunk

        def before(other, total):
            first_c = pl.multiple_of(other * chunk, chunk)
            return total + jnp.dot(
                parts_ref[:, pl.ds(first_c, chunk)],
                mask_block(first_c, first_r, False),
                preferred_element_type=F32,
            )

        total = jnp.dot(
            parts_ref[:, first_r : first_r + chunk],
            mask_block(first_r, first_r, True),
            preferred_element_type=F32,
        )
        total = lax.fori_loop(0, number, before, total)
        out_ref[0:features, first_r : first_r + chunk] = (
            total[0:features] + total[features : 2 * features]
        )
        out_ref[features:, first_r : first_r + chunk] = total[2 * features : 2 * features + EXTRA]


def final_kernel(flip_ref, key_ref, local_ref, state_ref, out_ref, table_ref):
    owners = state_ref.shape[0]
    events, features = out_ref.shape
    rows = table_ref.shape[0]
    flip = flip_ref[0]
    group = min(8, owners)
    ids = sublane_ids()
    per_chunk = events // LANES

    @pl.when(pl.program_id(0) == 0)
    def fill():
        def one(owner, carry):
            place = jnp.bitwise_xor(owner, flip)
            high, low = split_two(state_ref[place, 0:features, :])
            span = pl.ds(pl.multiple_of(owner * ACCOUNTS, ACCOUNTS), ACCOUNTS)
            table_ref[0:features, span] = high
            table_ref[features : 2 * features, span] = low
            count = state_ref[place, features : features + 1, :].astype(I32)
            digit = lax.broadcasted_iota(I32, (rows - 2 * features, LANES), 0)
            extra = jnp.where(
                digit == 0,
                count // 65536,
                jnp.where(digit == 1, (count // 256) % 256, jnp.where(digit == 2, count % 256, 0)),
            )
            table_ref[2 * features : rows, span] = extra.astype(F32).astype(BF16)
            return carry

        lax.fori_loop(0, owners, one, 0)

    first = pl.program_id(0) * per_chunk
    key = key_ref[pl.ds(pl.multiple_of(first, per_chunk), per_chunk), :]

    def part(number, total):
        lines = []
        for i in range(group):
            offset = (number * group + i) * ACCOUNTS
            mine = (key - offset).astype(F32)
            pieces = [
                jnp.where(mine[tile : tile + 1] == ids, 1.0, 0.0).astype(BF16)
                for tile in range(per_chunk)
            ]
            lines.append(jnp.concatenate(pieces, axis=1))
        block = jnp.concatenate(lines, axis=0)
        span = pl.ds(pl.multiple_of(number * group * ACCOUNTS, LANES), group * ACCOUNTS)
        return total + jnp.dot(table_ref[:, span], block, preferred_element_type=F32)

    zero = jnp.zeros((rows, events), F32)
    if owners == group:
        total = part(0, zero)
    else:
        total = lax.fori_loop(0, owners // group, part, zero)
    more = total[2 * features : 2 * features + 3]
    count = local_ref[features : features + 1, :] + (
        more[0:1] * 65536.0 + more[1:2] * 256.0 + more[2:3]
    )
    sums = local_ref[0:features, :] + (total[0:features] + total[features : 2 * features])
    out_ref[...] = (sums / count).T


VMEM = pl.BlockSpec(memory_space=pltpu.VMEM)
SMEM = pl.BlockSpec(memory_space=pltpu.SMEM)
PARAMS = pltpu.CompilerParams(vmem_limit_bytes=48 * 1024 * 1024)


def closing_states(flip, home, account, flags, features, owners):
    events, width = features.shape
    return pl.pallas_call(
        closing_kernel,
        out_shape=jax.ShapeDtypeStruct((owners, width + EXTRA, LANES), F32),
        in_specs=[SMEM, VMEM, VMEM, VMEM, VMEM],
        out_specs=VMEM,
        scratch_shapes=[
            pltpu.VMEM((events, 2 * width), BF16),
            pltpu.VMEM((max(8, owners), LANES), F32),
        ],
        compiler_params=PARAMS,
        name="closing",
    )(flip, home, account, flags, features)


def local_sums(home, account, flags, features):
    events, width = features.shape
    tiles = home.shape[0]
    return pl.pallas_call(
        local_kernel,
        out_shape=(
            jax.ShapeDtypeStruct((width + EXTRA, events), F32),
            jax.ShapeDtypeStruct((tiles, LANES), I32),
        ),
        in_specs=[VMEM, VMEM, VMEM, VMEM],
        out_specs=(VMEM, VMEM),
        scratch_shapes=[
            pltpu.VMEM((2 * width + 16, events), BF16),
            pltpu.VMEM((events, LANES), F32),
            pltpu.VMEM((tiles, LANES), F32),
            pltpu.VMEM((tiles, LANES), F32),
        ],
        compiler_params=PARAMS,
        name="local",
    )(home, account, flags, features)


def final_means(flip, key, local, state, events, width):
    chunk = min(1024, events)
    owners = state.shape[0]
    return pl.pallas_call(
        final_kernel,
        out_shape=jax.ShapeDtypeStruct((events, width), F32),
        grid=(events // chunk,),
        in_specs=[
            SMEM,
            VMEM,
            pl.BlockSpec((width + EXTRA, chunk), lambda i: (0, i)),
            VMEM,
        ],
        out_specs=pl.BlockSpec((chunk, width), lambda i: (i, 0)),
        scratch_shapes=[pltpu.VMEM((2 * width + 16, owners * ACCOUNTS), BF16)],
        compiler_params=PARAMS,
        name="final",
    )(flip, key, local, state)


def combine(earlier, later, mark):
    return later + (1.0 - later[:, mark : mark + 1, :]) * earlier


def scan_states(state, me, devices, width):
    mark = width + 1
    steps = devices.bit_length() - 1
    halvings = min(HALVINGS, steps, state.shape[0].bit_length() - 1)

    def swap(value, step):
        return lax.ppermute(value, AXES, [(i, i ^ (1 << step)) for i in range(devices)])

    kept = []
    for step in range(halvings):
        half = state.shape[0] // 2
        got = swap(state[half:], step)
        mine = state[:half]
        upper = ((me >> step) & 1) == 1
        low, high = jnp.where(upper, got, mine), jnp.where(upper, mine, got)
        kept.append((upper, low))
        state = combine(low, high, mark)
    before = jnp.zeros_like(state)
    for step in range(halvings, steps):
        got = swap(state, step)
        upper = ((me >> step) & 1) == 1
        before = jnp.where(upper, combine(got, before, mark), before)
        low, high = jnp.where(upper, got, state), jnp.where(upper, state, got)
        state = combine(low, high, mark)
    for step in range(halvings - 1, -1, -1):
        upper, low = kept[step]
        after = combine(before, low, mark)
        mine, theirs = jnp.where(upper, after, before), jnp.where(upper, before, after)
        before = jnp.concatenate([mine, swap(theirs, step)], axis=0)
    return before


def flip_of(me, devices, owners):
    bits = owners.bit_length() - 1
    flip = jnp.zeros((), I32)
    for step in range(min(HALVINGS, devices.bit_length() - 1, bits)):
        flip = flip | (((me >> step) & 1) << (bits - 1 - step))
    return flip.reshape(1)


def body(features, home, account, flags):
    owners = lax.axis_size("users")
    devices = lax.axis_size("tm") * owners
    events, width = features.shape
    tiles = events // LANES
    me = lax.axis_index("tm") * owners + lax.axis_index("users")
    flip = flip_of(me, devices, owners)
    home2 = home.reshape(tiles, LANES)
    account2 = account.reshape(tiles, LANES)
    flags2 = flags.reshape(tiles, LANES)
    state = closing_states(flip, home2, account2, flags2, features, owners)
    local, key = local_sums(home2, account2, flags2, features)
    before = scan_states(state, me, devices, width)
    return final_means(flip, key, local, before, events, width)


def solution(mesh):
    return jax.shard_map(
        body,
        mesh=mesh,
        in_specs=(P(AXES, None), P(AXES, None), P(AXES), P(AXES)),
        out_specs=P(AXES, None),
        check_vma=False,
    )
```

```python
import functools

import jax
import jax.numpy as jnp
from jax import lax
from jax.experimental import pallas as pl
from jax.experimental.pallas import tpu as pltpu
from jax.sharding import PartitionSpec as P


ACCOUNTS = 128
LANES = 128
EXTRA = 8
LEVELS = (1, 2)
STARTS = (0, 4, 6)
AXES = ("tm", "users")
F32, BF16, I32 = jnp.float32, jnp.bfloat16, jnp.int32


def split_two(x):
    high = x.astype(BF16)
    return high, (x - high.astype(F32)).astype(BF16)


def account_ids():
    return lax.broadcasted_iota(I32, (ACCOUNTS, LANES), 0).astype(F32).astype(BF16)


def row_positions(tiles):
    shape = (tiles, LANES)
    return lax.broadcasted_iota(I32, shape, 0) * LANES + lax.broadcasted_iota(I32, shape, 1)


def small(value):
    return jnp.asarray(value, BF16)


def closing_kernel(
    flip_ref,
    home_hbm,
    account_hbm,
    flag_hbm,
    x_hbm,
    out_ref,
    home_ref,
    account_ref,
    flag_ref,
    x_ref,
    parts_ref,
    last_ref,
    sems,
):
    pairs = (
        (home_hbm, home_ref),
        (account_hbm, account_ref),
        (flag_hbm, flag_ref),
        (x_hbm, x_ref),
    )
    copies = [pltpu.make_async_copy(a, b, sems.at[i]) for i, (a, b) in enumerate(pairs)]
    for copy in copies:
        copy.start()
    tiles = home_ref.shape[0]
    owners, rows = out_ref.shape[0], out_ref.shape[1]
    events, features = x_ref.shape
    chunk = min(512, events)
    group = 2 if owners % 2 == 0 else 1
    flip = flip_ref[0]
    ids = account_ids()
    lane = lax.broadcasted_iota(I32, (ACCOUNTS, LANES), 1).astype(F32)
    for copy in copies[:3]:
        copy.wait()
    home = home_ref[...]
    account = account_ref[...]
    flag = flag_ref[...]
    account_f = account.astype(F32)

    def find_last(owner, carry):
        kept = jnp.where((home == owner) & (flag == 1), account_f, -1.0).astype(BF16)
        latest = jnp.full((ACCOUNTS, LANES), -1.0, BF16)
        for tile in range(tiles):
            latest = jnp.where(kept[tile : tile + 1] == ids, small(tile), latest)
        latest = latest.astype(F32)
        place = jnp.where(latest >= 0.0, latest * LANES + lane, -1.0)
        last_ref[pl.ds(owner, 1), :] = jnp.max(place.T, axis=0, keepdims=True)
        return carry

    lax.fori_loop(0, owners, find_last, 0, unroll=min(owners, 8))

    def look_up(owner, least):
        row = jnp.broadcast_to(last_ref[pl.ds(owner, 1), :], (tiles, LANES))
        return jnp.where(home == owner, jnp.take_along_axis(row, account, axis=1), least)

    least = jnp.full((tiles, LANES), -1.0, F32)
    least = lax.fori_loop(0, owners, look_up, least, unroll=min(owners, 8))
    live = row_positions(tiles).astype(F32) >= least
    weight = jnp.where(flag == 1, 65.0, 1.0).astype(BF16)

    copies[3].wait()
    high, low = split_two(x_ref[...])
    parts_ref[:, 0:features] = high
    parts_ref[:, features : 2 * features] = low

    def one_group(number, carry):
        kept = [
            jnp.where(live & (home == number * group + i), account_f, -1.0).astype(BF16)
            for i in range(group)
        ]
        total = jnp.zeros((group * ACCOUNTS, 2 * features), F32)
        counts = [jnp.zeros((ACCOUNTS, LANES), BF16) for _ in range(group)]
        for first in range(0, events, chunk):
            blocks = []
            for i in range(group):
                pieces = []
                for tile in range(first // LANES, (first + chunk) // LANES):
                    mask = kept[i][tile : tile + 1] == ids
                    share = jnp.broadcast_to(weight[tile : tile + 1], mask.shape)
                    counts[i] = counts[i] + jnp.where(mask, share, small(0.0))
                    pieces.append(jnp.where(mask, small(1.0), small(0.0)))
                blocks.append(jnp.concatenate(pieces, axis=1))
            total = total + jnp.dot(
                jnp.concatenate(blocks, axis=0),
                parts_ref[first : first + chunk, :],
                preferred_element_type=F32,
            )
        sums = total[:, 0:features] + total[:, features : 2 * features]
        for i in range(group):
            place = jnp.bitwise_xor(number * group + i, flip)
            out_ref[place, 0:features, :] = sums[i * ACCOUNTS : (i + 1) * ACCOUNTS].T
            count = counts[i].astype(F32)
            count = jnp.where(count >= 64.0, count + (8192.0 - 64.0), count)
            tally = jnp.sum(count.T, axis=0, keepdims=True)
            marked = jnp.where(tally >= 8192.0, 1.0, 0.0)
            spot = lax.broadcasted_iota(I32, (rows - features, LANES), 0)
            out_ref[place, features:rows, :] = jnp.where(
                spot == 0, tally - 8192.0 * marked, jnp.where(spot == 1, marked, 0.0)
            )
        return carry

    lax.fori_loop(0, owners // group, one_group, 0, unroll=min(owners // group, 4))


def turn(row):
    return jnp.broadcast_to(row, (LANES, LANES)).T


def parts_kernel(x_ref, parts_ref):
    events, features = x_ref.shape
    rows = parts_ref.shape[0]
    for first in range(0, events, LANES):
        span = slice(first, first + LANES)
        high, low = split_two(x_ref[span, :].T)
        parts_ref[0:features, span] = high
        parts_ref[features : 2 * features, span] = low
    extra = lax.broadcasted_iota(I32, (rows - 2 * features, events), 0)
    parts_ref[2 * features : rows, :] = jnp.where(extra == 0, 1.0, 0.0).astype(BF16)


def stats_kernel(home_ref, account_ref, flag_ref, column_ref, sid_ref, key_ref, start_ref):
    tiles = home_ref.shape[0]
    events = tiles * LANES
    user = home_ref[...] * ACCOUNTS + account_ref[...]
    user_f = user.astype(F32)
    flagged = jnp.where(flag_ref[...] == 1, user_f, -1.0)
    row_id = lax.broadcasted_iota(I32, (LANES, LANES), 0)
    reaches = row_id <= lax.broadcasted_iota(I32, (LANES, LANES), 1)
    spot = row_id.astype(F32)
    for tile in range(tiles):
        column_ref[tile * LANES : (tile + 1) * LANES, :] = turn(flagged[tile : tile + 1])

    wide = 4 if tiles % 4 == 0 else 1
    for first in range(0, tiles, wide):
        mine = [user_f[first + i : first + i + 1] for i in range(wide)]

        def earlier(other, latest):
            column = column_ref[pl.ds(pl.multiple_of(other * LANES, LANES), LANES), :]
            place = spot + (other * LANES).astype(F32)
            return tuple(jnp.where(column == mine[i], place, latest[i]) for i in range(wide))

        latest = tuple(jnp.full((LANES, LANES), -1.0, F32) for _ in range(wide))
        latest = list(lax.fori_loop(0, first, earlier, latest))
        for i in range(wide):
            for other in range(first, first + i + 1):
                column = column_ref[other * LANES : (other + 1) * LANES, :]
                mask = column == mine[i]
                if other == first + i:
                    mask = mask & reaches
                latest[i] = jnp.where(mask, spot + float(other * LANES), latest[i])
            start_ref[first + i : first + i + 1, :] = jnp.max(latest[i], axis=0, keepdims=True)
    start = start_ref[...]
    key_ref[...] = jnp.where(start < 0.0, user, -1)
    sid = jnp.where(start < 0.0, user_f + float(events), start)
    sid_ref[...] = sid
    for tile in range(tiles):
        column_ref[tile * LANES : (tile + 1) * LANES, :] = turn(sid[tile : tile + 1])


def local_kernel(parts_ref, column_ref, sid_ref, out_ref, mask_ref, *, first, chunk):
    features = out_ref.shape[0] - EXTRA
    reaches = lax.broadcasted_iota(I32, (LANES, LANES), 0) <= lax.broadcasted_iota(
        I32, (LANES, LANES), 1
    )
    sid = sid_ref[...]
    for begin in range(first, first + out_ref.shape[1], chunk):
        slot = (begin // chunk) % 2
        depth = begin + chunk
        lines = [sid[t : t + 1] for t in range(begin // LANES, depth // LANES)]
        for c in range(0, depth, LANES):
            column = column_ref[c : c + LANES, :]
            for i, line in enumerate(lines):
                r = begin + i * LANES
                if c > r:
                    block = jnp.zeros((LANES, LANES), BF16)
                else:
                    mask = column == line
                    if c == r:
                        mask = mask & reaches
                    block = jnp.where(mask, 1.0, 0.0).astype(BF16)
                mask_ref[slot, c : c + LANES, i * LANES : (i + 1) * LANES] = block
        total = jnp.dot(
            parts_ref[:, 0:depth], mask_ref[slot, 0:depth, :], preferred_element_type=F32
        )
        span = slice(begin - first, begin - first + chunk)
        out_ref[0:features, span] = total[0:features] + total[features : 2 * features]
        out_ref[features:, span] = total[2 * features : 2 * features + EXTRA]


def final_kernel(flip_ref, key_ref, state_ref, *refs, starts, chunk):
    local_refs, out_ref, table_ref = refs[: len(starts)], refs[-4], refs[-3]
    stage_ref, sems = refs[-2], refs[-1]
    owners = state_ref.shape[0]
    events, features = out_ref.shape
    rows = table_ref.shape[0]
    flip = flip_ref[0]
    group = min(8, owners)
    ids = account_ids()

    def fill(owner, carry):
        place = jnp.bitwise_xor(owner, flip)
        high, low = split_two(state_ref[place, 0:features, :])
        span = pl.ds(pl.multiple_of(owner * ACCOUNTS, ACCOUNTS), ACCOUNTS)
        table_ref[0:features, span] = high
        table_ref[features : 2 * features, span] = low
        count = state_ref[place, features : features + 1, :].astype(I32)
        digit = lax.broadcasted_iota(I32, (rows - 2 * features, LANES), 0)
        extra = jnp.where(
            digit == 0,
            lax.shift_right_logical(count, 16),
            jnp.where(
                digit == 1,
                lax.shift_right_logical(count, 8) & 255,
                jnp.where(digit == 2, count & 255, 0),
            ),
        )
        table_ref[2 * features : rows, span] = extra.astype(F32).astype(BF16)
        return carry

    lax.fori_loop(0, owners, fill, 0, unroll=min(owners, 8))

    key = key_ref[...]
    account_f = (key & (ACCOUNTS - 1)).astype(F32)
    home = lax.shift_right_arithmetic(key, ACCOUNTS.bit_length() - 1)
    copies = []
    for begin in range(0, events, chunk):
        number = begin // chunk
        piece = max(i for i in range(len(starts)) if starts[i] <= begin)
        local_ref = local_refs[piece]
        span = slice(begin - starts[piece], begin - starts[piece] + chunk)

        def part(step, total):
            lines = []
            for i in range(group):
                mine = jnp.where(home == step * group + i, account_f, -1.0).astype(BF16)
                blocks = [
                    jnp.where(mine[tile : tile + 1] == ids, small(1.0), small(0.0))
                    for tile in range(begin // LANES, (begin + chunk) // LANES)
                ]
                lines.append(jnp.concatenate(blocks, axis=1))
            place = pl.ds(pl.multiple_of(step * group * ACCOUNTS, LANES), group * ACCOUNTS)
            found = jnp.dot(
                table_ref[:, place], jnp.concatenate(lines, axis=0), preferred_element_type=F32
            )
            return found if total is None else total + found

        if owners == group:
            total = part(0, None)
        else:
            total = lax.fori_loop(0, owners // group, part, jnp.zeros((rows, chunk), F32))
        more = total[2 * features : 2 * features + 3]
        count = local_ref[features : features + 1, span] + (
            more[0:1] * 65536.0 + more[1:2] * 256.0 + more[2:3]
        )
        sums = local_ref[0:features, span] + (total[0:features] + total[features : 2 * features])
        stage_ref[begin : begin + chunk, :] = (sums * (1.0 / count)).T
        copy = pltpu.make_async_copy(
            stage_ref.at[pl.ds(begin, chunk), :],
            out_ref.at[pl.ds(begin, chunk), :],
            sems.at[number],
        )
        copy.start()
        copies.append(copy)
    for copy in copies:
        copy.wait()


VMEM = pl.BlockSpec(memory_space=pltpu.VMEM)
SMEM = pl.BlockSpec(memory_space=pltpu.SMEM)
HBM = pl.BlockSpec(memory_space=pltpu.HBM)
PARAMS = pltpu.CompilerParams(vmem_limit_bytes=28 * 1024 * 1024)


def closing_states(flip, home, account, flags, features, owners):
    events, width = features.shape
    tiles = events // LANES
    home, account, flags, features = [
        pltpu.with_memory_space_constraint(v, pltpu.HBM) for v in (home, account, flags, features)
    ]
    return pl.pallas_call(
        closing_kernel,
        out_shape=jax.ShapeDtypeStruct((owners, width + EXTRA, LANES), F32),
        in_specs=[SMEM, HBM, HBM, HBM, HBM],
        out_specs=VMEM,
        scratch_shapes=[pltpu.VMEM((tiles, LANES), I32)] * 3
        + [
            pltpu.VMEM((events, width), F32),
            pltpu.VMEM((events, 2 * width), BF16),
            pltpu.VMEM((max(8, owners), LANES), F32),
            pltpu.SemaphoreType.DMA((4,)),
        ],
        compiler_params=PARAMS,
        name="closing",
    )(flip, home, account, flags, features)


def feature_parts(features):
    events, width = features.shape
    return pl.pallas_call(
        parts_kernel,
        out_shape=jax.ShapeDtypeStruct((2 * width + 16, events), BF16),
        in_specs=[VMEM],
        out_specs=VMEM,
        compiler_params=PARAMS,
        name="parts",
    )(features)


def event_stats(home, account, flags):
    tiles = home.shape[0]
    return pl.pallas_call(
        stats_kernel,
        out_shape=(
            jax.ShapeDtypeStruct((tiles * LANES, LANES), F32),
            jax.ShapeDtypeStruct((tiles, LANES), F32),
            jax.ShapeDtypeStruct((tiles, LANES), I32),
        ),
        in_specs=[VMEM, VMEM, VMEM],
        out_specs=(VMEM, VMEM, VMEM),
        scratch_shapes=[pltpu.VMEM((tiles, LANES), F32)],
        compiler_params=PARAMS,
        name="stats",
    )(home, account, flags)


def local_sums(parts, column, sid, first, length, width):
    chunk = min(512, length)
    return pl.pallas_call(
        functools.partial(local_kernel, first=first, chunk=chunk),
        out_shape=jax.ShapeDtypeStruct((width + EXTRA, length), F32),
        in_specs=[VMEM, VMEM, VMEM],
        out_specs=VMEM,
        scratch_shapes=[pltpu.VMEM((2, first + length, chunk), BF16)],
        compiler_params=PARAMS,
        name="local",
    )(parts, column, sid)


def final_means(flip, key, state, pieces, starts, events, width):
    chunk = min(512, events)
    owners = state.shape[0]
    return pl.pallas_call(
        functools.partial(final_kernel, starts=starts, chunk=chunk),
        out_shape=jax.ShapeDtypeStruct((events, width), F32),
        in_specs=[SMEM, VMEM, VMEM] + [VMEM] * len(pieces),
        out_specs=HBM,
        scratch_shapes=[
            pltpu.VMEM((2 * width + 16, owners * ACCOUNTS), BF16),
            pltpu.VMEM((events, width), F32),
            pltpu.SemaphoreType.DMA((events // chunk,)),
        ],
        compiler_params=PARAMS,
        name="final",
    )(flip, key, state, *pieces)


def combine(earlier, later, mark):
    return later + (1.0 - later[:, mark : mark + 1, :]) * earlier


def pick(parts, bits):
    for place, bit in enumerate(bits):
        step = 1 << place
        parts = [jnp.where(bit, parts[i ^ step], parts[i]) for i in range(len(parts))]
    return parts


def levels_of(devices, owners):
    left, levels = min(devices, owners).bit_length() - 1, []
    for want in LEVELS:
        if left > 0:
            levels.append(min(want, left))
            left -= levels[-1]
    return levels


def scan_states(state, me, devices, width, levels):
    mark = width + 1
    steps = devices.bit_length() - 1

    def swap(value, mask):
        return lax.ppermute(value, AXES, [(i, i ^ mask) for i in range(devices)])

    def bit(step):
        return ((me >> step) & 1) == 1

    saved, done = [], 0
    for level in levels:
        part = state.shape[0] >> level
        got = [state[:part]]
        for other in range(1, 1 << level):
            piece = state[other * part : (other + 1) * part]
            got.append(swap(piece, other << done))
        bits = [bit(done + i) for i in range(level)]
        ordered = pick(got, bits)
        saved.append((done, bits, ordered))
        state = ordered[0]
        for later in ordered[1:]:
            state = combine(state, later, mark)
        done += level
    before = jnp.zeros_like(state)
    for step in range(done, steps):
        got = swap(state, 1 << step)
        before = jnp.where(bit(step), combine(got, before, mark), before)
        if step < steps - 1:
            low, high = jnp.where(bit(step), got, state), jnp.where(bit(step), state, got)
            state = combine(low, high, mark)
    for done, bits, ordered in reversed(saved):
        prefixes = [before]
        for earlier in ordered[:-1]:
            prefixes.append(combine(prefixes[-1], earlier, mark))
        mine = pick(prefixes, bits)
        got = [mine[0]]
        for other in range(1, len(mine)):
            got.append(swap(mine[other], other << done))
        before = jnp.concatenate(got, axis=0)
    return before


def flip_of(me, levels, owners):
    flip, done, top = jnp.zeros((), I32), 0, owners.bit_length() - 1
    for level in levels:
        top -= level
        flip = flip | (((me >> done) & ((1 << level) - 1)) << top)
        done += level
    return flip.reshape(1)


def body(features, home, account, flags):
    owners = lax.axis_size("users")
    devices = lax.axis_size("tm") * owners
    events, width = features.shape
    tiles = events // LANES
    me = lax.axis_index("tm") * owners + lax.axis_index("users")
    levels = levels_of(devices, owners)
    flip = flip_of(me, levels, owners)
    home2 = home.reshape(tiles, LANES)
    account2 = account.reshape(tiles, LANES)
    flags2 = flags.reshape(tiles, LANES)
    state = closing_states(flip, home2, account2, flags2, features, owners)
    column, sid, key = event_stats(home2, account2, flags2)
    parts = feature_parts(features)
    starts = [events * i // 8 for i in STARTS]
    pieces = []
    for i, first in enumerate(starts):
        length = (starts + [events])[i + 1] - first
        pieces.append(local_sums(parts, column, sid, first, length, width))
    before = scan_states(state, me, devices, width, levels)
    return final_means(flip, key, before, pieces, starts, events, width)


def solution(mesh):
    return jax.shard_map(
        body,
        mesh=mesh,
        in_specs=(P(AXES, None), P(AXES, None), P(AXES), P(AXES)),
        out_specs=P(AXES, None),
        check_vma=False,
    )
```

```python
import functools

import jax
import jax.numpy as jnp
from jax import lax
from jax.experimental import pallas as pl
from jax.experimental.pallas import tpu as pltpu
from jax.sharding import PartitionSpec as P


ACCOUNTS = 128
LANES = 128
EXTRA = 8
LEVELS = (1, 2)
STARTS = (0, 3, 5, 7)
AXES = ("tm", "users")
F32, BF16, I32 = jnp.float32, jnp.bfloat16, jnp.int32


def split_two(x):
    high = x.astype(BF16)
    return high, (x - high.astype(F32)).astype(BF16)


def account_ids():
    return lax.broadcasted_iota(I32, (ACCOUNTS, LANES), 0).astype(F32).astype(BF16)


def row_positions(tiles):
    shape = (tiles, LANES)
    return lax.broadcasted_iota(I32, shape, 0) * LANES + lax.broadcasted_iota(I32, shape, 1)


def small(value):
    return jnp.asarray(value, BF16)


def closing_kernel(
    flip_ref,
    home_hbm,
    account_hbm,
    flag_hbm,
    x_hbm,
    kept_ref,
    sent_ref,
    home_ref,
    account_ref,
    flag_ref,
    x_ref,
    parts_ref,
    last_ref,
    sems,
):
    pairs = (
        (home_hbm, home_ref),
        (account_hbm, account_ref),
        (flag_hbm, flag_ref),
        (x_hbm, x_ref),
    )
    copies = [pltpu.make_async_copy(a, b, sems.at[i]) for i, (a, b) in enumerate(pairs)]
    for copy in copies:
        copy.start()
    for copy in copies[:3]:
        copy.wait()
    home, account, flag = home_ref[...], account_ref[...], flag_ref[...]
    flip = flip_ref[0]
    tiles = home.shape[0]
    half, rows = kept_ref.shape[0], kept_ref.shape[1]
    slots = 2 * half
    events, features = x_ref.shape
    chunk = min(512, events)
    group = 2 if half % 2 == 0 else 1
    ids = account_ids()
    lane = lax.broadcasted_iota(I32, (ACCOUNTS, LANES), 1).astype(F32)
    account_f = account.astype(F32)

    def owner_of(slot):
        return jnp.bitwise_xor(slot, flip)

    def find_last(slot, carry):
        kept = jnp.where((home == owner_of(slot)) & (flag == 1), account_f, -1.0).astype(BF16)
        latest = jnp.full((ACCOUNTS, LANES), -1.0, BF16)
        for tile in range(tiles):
            latest = jnp.where(kept[tile : tile + 1] == ids, small(tile), latest)
        latest = latest.astype(F32)
        place = jnp.where(latest >= 0.0, latest * LANES + lane, -1.0)
        last_ref[pl.ds(slot, 1), :] = jnp.max(place.T, axis=0, keepdims=True)
        return carry

    lax.fori_loop(0, slots, find_last, 0, unroll=min(slots, 8))

    def look_up(slot, least):
        row = jnp.broadcast_to(last_ref[pl.ds(slot, 1), :], (tiles, LANES))
        found = jnp.take_along_axis(row, account, axis=1)
        return jnp.where(home == owner_of(slot), found, least)

    least = jnp.full((tiles, LANES), -1.0, F32)
    least = lax.fori_loop(0, slots, look_up, least, unroll=min(slots, 8))
    live = row_positions(tiles).astype(F32) >= least
    weight = jnp.where(flag == 1, 65.0, 1.0).astype(BF16)
    copies[3].wait()
    high, low = split_two(x_ref[...])
    parts_ref[:, 0:features] = high
    parts_ref[:, features : 2 * features] = low

    def one_group(number, out_ref, base):
        kept = [
            jnp.where(live & (home == owner_of(base + number * group + i)), account_f, -1.0).astype(BF16)
            for i in range(group)
        ]
        total = jnp.zeros((group * ACCOUNTS, 2 * features), F32)
        counts = [jnp.zeros((ACCOUNTS, LANES), BF16) for _ in range(group)]
        for begin in range(0, events, chunk):
            blocks = []
            for i in range(group):
                pieces = []
                for tile in range(begin // LANES, (begin + chunk) // LANES):
                    mask = kept[i][tile : tile + 1] == ids
                    share = jnp.broadcast_to(weight[tile : tile + 1], mask.shape)
                    counts[i] = counts[i] + jnp.where(mask, share, small(0.0))
                    pieces.append(jnp.where(mask, small(1.0), small(0.0)))
                blocks.append(jnp.concatenate(pieces, axis=1))
            total = total + jnp.dot(
                jnp.concatenate(blocks, axis=0),
                parts_ref[begin : begin + chunk, :],
                preferred_element_type=F32,
            )
        sums = total[:, 0:features] + total[:, features : 2 * features]
        for i in range(group):
            place = number * group + i
            out_ref[place, 0:features, :] = sums[i * ACCOUNTS : (i + 1) * ACCOUNTS].T
            count = counts[i].astype(F32)
            count = jnp.where(count >= 64.0, count + (8192.0 - 64.0), count)
            tally = jnp.sum(count.T, axis=0, keepdims=True)
            marked = jnp.where(tally >= 8192.0, 1.0, 0.0)
            spot = lax.broadcasted_iota(I32, (rows - features, LANES), 0)
            out_ref[place, features:rows, :] = jnp.where(
                spot == 0, tally - 8192.0 * marked, jnp.where(spot == 1, marked, 0.0)
            )

    def both(number, carry):
        one_group(number, sent_ref, half)
        one_group(number, kept_ref, 0)
        return carry

    lax.fori_loop(0, half // group, both, 0, unroll=min(half // group, 2))


def turn(row):
    return jnp.broadcast_to(row, (LANES, LANES)).T


def parts_kernel(x_ref, parts_ref):
    events, features = x_ref.shape
    rows = parts_ref.shape[0]
    for first in range(0, events, LANES):
        span = slice(first, first + LANES)
        high, low = split_two(x_ref[span, :].T)
        parts_ref[0:features, span] = high
        parts_ref[features : 2 * features, span] = low
    extra = lax.broadcasted_iota(I32, (rows - 2 * features, events), 0)
    parts_ref[2 * features : rows, :] = jnp.where(extra == 0, 1.0, 0.0).astype(BF16)


def stats_kernel(home_ref, account_ref, flag_ref, column_ref, sid_ref, key_ref, start_ref):
    tiles = home_ref.shape[0]
    events = tiles * LANES
    user = home_ref[...] * ACCOUNTS + account_ref[...]
    user_f = user.astype(F32)
    flagged = jnp.where(flag_ref[...] == 1, user_f, -1.0)
    row_id = lax.broadcasted_iota(I32, (LANES, LANES), 0)
    reaches = row_id <= lax.broadcasted_iota(I32, (LANES, LANES), 1)
    spot = row_id.astype(F32)
    for tile in range(tiles):
        column_ref[tile * LANES : (tile + 1) * LANES, :] = turn(flagged[tile : tile + 1])

    wide = 2 if tiles % 2 == 0 else 1
    for first in range(0, tiles, wide):
        mine = [user_f[first + i : first + i + 1] for i in range(wide)]

        def earlier(step, latest):
            for other in [step * wide + i for i in range(wide)]:
                column = column_ref[pl.ds(pl.multiple_of(other * LANES, LANES), LANES), :]
                place = other.astype(F32)
                latest = tuple(jnp.where(column == mine[i], place, latest[i]) for i in range(wide))
            return latest

        latest = tuple(jnp.full((LANES, LANES), -1.0, F32) for _ in range(wide))
        latest = list(lax.fori_loop(0, first // wide, earlier, latest))
        for i in range(wide):
            for other in range(first, first + i + 1):
                column = column_ref[other * LANES : (other + 1) * LANES, :]
                mask = column == mine[i]
                if other == first + i:
                    mask = mask & reaches
                latest[i] = jnp.where(mask, float(other), latest[i])
            place = jnp.where(latest[i] < 0.0, -1.0, latest[i] * LANES + spot)
            start_ref[first + i : first + i + 1, :] = jnp.max(place, axis=0, keepdims=True)
    start = start_ref[...]
    key_ref[...] = jnp.where(start < 0.0, user, -1)
    sid = jnp.where(start < 0.0, user_f + float(events), start)
    sid_ref[...] = sid
    for tile in range(tiles):
        column_ref[tile * LANES : (tile + 1) * LANES, :] = turn(sid[tile : tile + 1])


def local_kernel(parts_ref, column_ref, sid_ref, out_ref, mask_ref, *, first, chunk):
    features = out_ref.shape[0] - EXTRA
    reaches = lax.broadcasted_iota(I32, (LANES, LANES), 0) <= lax.broadcasted_iota(
        I32, (LANES, LANES), 1
    )
    sid = sid_ref[...]
    for begin in range(first, first + out_ref.shape[1], chunk):
        slot = (begin // chunk) % 2
        depth = begin + chunk
        lines = [sid[t : t + 1] for t in range(begin // LANES, depth // LANES)]
        for c in range(0, depth, LANES):
            column = column_ref[c : c + LANES, :]
            for i, line in enumerate(lines):
                r = begin + i * LANES
                if c > r:
                    block = jnp.zeros((LANES, LANES), BF16)
                else:
                    mask = column == line
                    if c == r:
                        mask = mask & reaches
                    block = jnp.where(mask, 1.0, 0.0).astype(BF16)
                mask_ref[slot, c : c + LANES, i * LANES : (i + 1) * LANES] = block
        total = jnp.dot(
            parts_ref[:, 0:depth], mask_ref[slot, 0:depth, :], preferred_element_type=F32
        )
        span = slice(begin - first, begin - first + chunk)
        out_ref[0:features, span] = total[0:features] + total[features : 2 * features]
        out_ref[features:, span] = total[2 * features : 2 * features + EXTRA]


def gather_states(flip, first, key, state_ref, table_ref, chunk, finish):
    slots = state_ref.shape[0]
    events = key.shape[0] * LANES
    rows, features = table_ref.shape[0], state_ref.shape[1] - EXTRA
    group = min(8, slots)
    ids = account_ids()

    def fill(slot, carry):
        high, low = split_two(state_ref[slot, 0:features, :])
        span = pl.ds(pl.multiple_of(slot * ACCOUNTS, ACCOUNTS), ACCOUNTS)
        table_ref[0:features, span] = high
        table_ref[features : 2 * features, span] = low
        count = state_ref[slot, features : features + 1, :].astype(I32)
        digit = lax.broadcasted_iota(I32, (rows - 2 * features, LANES), 0)
        extra = jnp.where(
            digit == 0,
            lax.shift_right_logical(count, 16),
            jnp.where(
                digit == 1,
                lax.shift_right_logical(count, 8) & 255,
                jnp.where(digit == 2, count & 255, 0),
            ),
        )
        table_ref[2 * features : rows, span] = extra.astype(F32).astype(BF16)
        return carry

    lax.fori_loop(0, slots, fill, 0, unroll=min(slots, 8))
    account_f = (key & (ACCOUNTS - 1)).astype(F32)
    home = lax.shift_right_arithmetic(key, ACCOUNTS.bit_length() - 1)

    for begin in range(0, events, chunk):

        def part(step, total):
            lines = []
            for i in range(group):
                owner = jnp.bitwise_xor(first + step * group + i, flip)
                mine = jnp.where(home == owner, account_f, -1.0).astype(BF16)
                blocks = [
                    jnp.where(mine[tile : tile + 1] == ids, small(1.0), small(0.0))
                    for tile in range(begin // LANES, (begin + chunk) // LANES)
                ]
                lines.append(jnp.concatenate(blocks, axis=1))
            place = pl.ds(pl.multiple_of(step * group * ACCOUNTS, LANES), group * ACCOUNTS)
            found = jnp.dot(
                table_ref[:, place], jnp.concatenate(lines, axis=0), preferred_element_type=F32
            )
            return found if total is None else total + found

        if slots == group:
            total = part(0, None)
        else:
            total = lax.fori_loop(0, slots // group, part, jnp.zeros((rows, chunk), F32))
        more = total[2 * features : 2 * features + 3]
        count = more[0:1] * 65536.0 + more[1:2] * 256.0 + more[2:3]
        finish(begin, total[0:features] + total[features : 2 * features], count)


def gather_kernel(flip_ref, key_ref, state_ref, *refs, starts, chunk, first):
    local_refs, out_ref, table_ref = refs[: len(starts)], refs[-2], refs[-1]
    features = state_ref.shape[1] - EXTRA

    def finish(begin, sums, count):
        piece = max(i for i in range(len(starts)) if starts[i] <= begin)
        local_ref = local_refs[piece]
        span = slice(begin - starts[piece], begin - starts[piece] + chunk)
        out_ref[0:features, begin : begin + chunk] = local_ref[0:features, span] + sums
        out_ref[features : features + 1, begin : begin + chunk] = (
            local_ref[features : features + 1, span] + count
        )

    gather_states(flip_ref[0], first, key_ref[...], state_ref, table_ref, chunk, finish)


def final_kernel(
    flip_ref, key_ref, state_ref, sums_ref, out_ref, table_ref, stage_ref, sems, *, chunk, first
):
    features = state_ref.shape[1] - EXTRA
    copies = []

    def finish(begin, sums, count):
        span = slice(begin, begin + chunk)
        sums = sums_ref[0:features, span] + sums
        count = sums_ref[features : features + 1, span] + count
        stage_ref[span, :] = (sums * (1.0 / count)).T
        rows = pl.ds(begin, chunk)
        copy = pltpu.make_async_copy(
            stage_ref.at[rows, :], out_ref.at[rows, :], sems.at[begin // chunk]
        )
        copy.start()
        copies.append(copy)

    gather_states(flip_ref[0], first, key_ref[...], state_ref, table_ref, chunk, finish)
    for copy in copies:
        copy.wait()


VMEM = pl.BlockSpec(memory_space=pltpu.VMEM)
SMEM = pl.BlockSpec(memory_space=pltpu.SMEM)
HBM = pl.BlockSpec(memory_space=pltpu.HBM)
PARAMS = pltpu.CompilerParams(vmem_limit_bytes=28 * 1024 * 1024)


def closing_states(flip, home, account, flags, features, owners):
    events, width = features.shape
    tiles = events // LANES
    home, account, flags, features = [
        pltpu.with_memory_space_constraint(v, pltpu.HBM) for v in (home, account, flags, features)
    ]
    shape = jax.ShapeDtypeStruct((owners // 2, width + EXTRA, LANES), F32)
    return pl.pallas_call(
        closing_kernel,
        out_shape=(shape, shape),
        in_specs=[SMEM, HBM, HBM, HBM, HBM],
        out_specs=(VMEM, VMEM),
        scratch_shapes=[pltpu.VMEM((tiles, LANES), I32)] * 3
        + [
            pltpu.VMEM((events, width), F32),
            pltpu.VMEM((events, 2 * width), BF16),
            pltpu.VMEM((max(8, owners), LANES), F32),
            pltpu.SemaphoreType.DMA((4,)),
        ],
        compiler_params=PARAMS,
        name="closing",
    )(flip, home, account, flags, features)


def feature_parts(features):
    events, width = features.shape
    return pl.pallas_call(
        parts_kernel,
        out_shape=jax.ShapeDtypeStruct((2 * width + 16, events), BF16),
        in_specs=[VMEM],
        out_specs=VMEM,
        compiler_params=PARAMS,
        name="parts",
    )(features)


def event_stats(home, account, flags):
    tiles = home.shape[0]
    return pl.pallas_call(
        stats_kernel,
        out_shape=(
            jax.ShapeDtypeStruct((tiles * LANES, LANES), F32),
            jax.ShapeDtypeStruct((tiles, LANES), F32),
            jax.ShapeDtypeStruct((tiles, LANES), I32),
        ),
        in_specs=[VMEM, VMEM, VMEM],
        out_specs=(VMEM, VMEM, VMEM),
        scratch_shapes=[pltpu.VMEM((tiles, LANES), F32)],
        compiler_params=PARAMS,
        name="stats",
    )(home, account, flags)


def local_sums(parts, column, sid, first, length, width):
    chunk = min(512, length)
    return pl.pallas_call(
        functools.partial(local_kernel, first=first, chunk=chunk),
        out_shape=jax.ShapeDtypeStruct((width + EXTRA, length), F32),
        in_specs=[VMEM, VMEM, VMEM],
        out_specs=VMEM,
        scratch_shapes=[pltpu.VMEM((2, first + length, chunk), BF16)],
        compiler_params=PARAMS,
        name="local",
    )(parts, column, sid)


def first_gather(flip, key, state, pieces, starts, events, width):
    chunk = min(512, events)
    return pl.pallas_call(
        functools.partial(gather_kernel, starts=starts, chunk=chunk, first=0),
        out_shape=jax.ShapeDtypeStruct((width + EXTRA, events), F32),
        in_specs=[SMEM, VMEM, VMEM] + [VMEM] * len(pieces),
        out_specs=VMEM,
        scratch_shapes=[pltpu.VMEM((2 * width + 16, state.shape[0] * ACCOUNTS), BF16)],
        compiler_params=PARAMS,
        name="gather",
    )(flip, key, state, *pieces)


def final_means(flip, key, state, sums, events, width, first):
    chunk = min(512, events)
    return pl.pallas_call(
        functools.partial(final_kernel, chunk=chunk, first=first),
        out_shape=jax.ShapeDtypeStruct((events, width), F32),
        in_specs=[SMEM, VMEM, VMEM, VMEM],
        out_specs=HBM,
        scratch_shapes=[
            pltpu.VMEM((2 * width + 16, state.shape[0] * ACCOUNTS), BF16),
            pltpu.VMEM((events, width), F32),
            pltpu.SemaphoreType.DMA((events // chunk,)),
        ],
        compiler_params=PARAMS,
        name="final",
    )(flip, key, state, sums)


def combine(earlier, later, mark):
    return later + (1.0 - later[:, mark : mark + 1, :]) * earlier


def pick(parts, bits):
    for place, bit in enumerate(bits):
        step = 1 << place
        parts = [jnp.where(bit, parts[i ^ step], parts[i]) for i in range(len(parts))]
    return parts


def levels_of(devices, owners):
    left, levels = min(devices, owners).bit_length() - 1, []
    for want in LEVELS:
        if left > 0:
            levels.append(min(want, left))
            left -= levels[-1]
    return levels


def scan_states(kept, sent, me, devices, width, levels):
    mark = width + 1
    state = None
    steps = devices.bit_length() - 1

    def swap(value, mask):
        return lax.ppermute(value, AXES, [(i, i ^ mask) for i in range(devices)])

    def bit(step):
        return ((me >> step) & 1) == 1

    saved, done = [], 0
    for level in levels:
        if done == 0:
            parts = [kept, sent]
        else:
            part = state.shape[0] >> level
            parts = [state[i * part : (i + 1) * part] for i in range(1 << level)]
        got = [parts[0]]
        for other in range(1, 1 << level):
            piece = parts[other]
            got.append(swap(piece, other << done))
        bits = [bit(done + i) for i in range(level)]
        ordered = pick(got, bits)
        saved.append((done, bits, ordered))
        state = ordered[0]
        for later in ordered[1:]:
            state = combine(state, later, mark)
        done += level
    before = jnp.zeros_like(state)
    while done < steps:
        level = min(2, steps - done)
        got = [state]
        for other in range(1, 1 << level):
            got.append(swap(state, other << done))
        bits = [bit(done + i) for i in range(level)]
        ordered = pick(got, bits)
        earlier = [jnp.zeros_like(state), ordered[0]]
        for later in ordered[1:-1]:
            earlier.append(combine(earlier[-1], later, mark))
        before = combine(pick(earlier, bits)[0], before, mark)
        done += level
        if done < steps:
            state = combine(earlier[-1], ordered[-1], mark)
    for done, bits, ordered in reversed(saved):
        prefixes = [before]
        for earlier in ordered[:-1]:
            prefixes.append(combine(prefixes[-1], earlier, mark))
        mine = pick(prefixes, bits)
        got = [mine[0]]
        for other in range(1, len(mine)):
            got.append(swap(mine[other], other << done))
        if done == 0:
            return got
        before = jnp.concatenate(got, axis=0)


def flip_of(me, levels, owners):
    flip, done, top = jnp.zeros((), I32), 0, owners.bit_length() - 1
    for level in levels:
        top -= level
        flip = flip | (((me >> done) & ((1 << level) - 1)) << top)
        done += level
    return flip.reshape(1)


def body(features, home, account, flags):
    owners = lax.axis_size("users")
    devices = lax.axis_size("tm") * owners
    events, width = features.shape
    tiles = events // LANES
    me = lax.axis_index("tm") * owners + lax.axis_index("users")
    levels = levels_of(devices, owners)
    flip = flip_of(me, levels, owners)
    home2 = home.reshape(tiles, LANES)
    account2 = account.reshape(tiles, LANES)
    flags2 = flags.reshape(tiles, LANES)
    half = owners // 2
    kept, sent = closing_states(flip, home2, account2, flags2, features, owners)
    column, sid, key = event_stats(home2, account2, flags2)
    parts = feature_parts(features)
    starts = [events * i // 8 for i in STARTS]
    pieces = []
    for i, first in enumerate(starts):
        length = (starts + [events])[i + 1] - first
        pieces.append(local_sums(parts, column, sid, first, length, width))
    mine, theirs = scan_states(kept, sent, me, devices, width, levels)
    sums = first_gather(flip, key, mine, pieces, starts, events, width)
    return final_means(flip, key, theirs, sums, events, width, half)


def solution(mesh):
    return jax.shard_map(
        body,
        mesh=mesh,
        in_specs=(P(AXES, None), P(AXES, None), P(AXES), P(AXES)),
        out_specs=P(AXES, None),
        check_vma=False,
    )
```

```python
import functools

import jax
import jax.numpy as jnp
from jax import lax
from jax.experimental import pallas as pl
from jax.experimental.pallas import tpu as pltpu
from jax.sharding import PartitionSpec as P


ACCOUNTS = 128
LANES = 128
EXTRA = 8
LEVELS = (1, 2)
STARTS = (0, 3, 5, 7)
AXES = ("tm", "users")
F32, BF16, I32 = jnp.float32, jnp.bfloat16, jnp.int32


def split_two(x):
    high = x.astype(BF16)
    return high, (x - high.astype(F32)).astype(BF16)


def account_ids():
    return lax.broadcasted_iota(I32, (ACCOUNTS, LANES), 0).astype(F32).astype(BF16)


def row_positions(tiles):
    shape = (tiles, LANES)
    return lax.broadcasted_iota(I32, shape, 0) * LANES + lax.broadcasted_iota(I32, shape, 1)


def small(value):
    return jnp.asarray(value, BF16)


def closing_kernel(
    flip_ref,
    home_hbm,
    account_hbm,
    flag_hbm,
    x_hbm,
    kept_ref,
    sent_ref,
    home_ref,
    account_ref,
    flag_ref,
    x_ref,
    parts_ref,
    last_ref,
    sems,
):
    pairs = (
        (home_hbm, home_ref),
        (account_hbm, account_ref),
        (flag_hbm, flag_ref),
        (x_hbm, x_ref),
    )
    copies = [pltpu.make_async_copy(a, b, sems.at[i]) for i, (a, b) in enumerate(pairs)]
    for copy in copies:
        copy.start()
    for copy in copies[:3]:
        copy.wait()
    home, account, flag = home_ref[...], account_ref[...], flag_ref[...]
    flip = flip_ref[0]
    tiles = home.shape[0]
    half, rows = kept_ref.shape[0], kept_ref.shape[1]
    slots = 2 * half
    events, features = x_ref.shape
    chunk = min(512, events)
    group = 2 if half % 2 == 0 else 1
    ids = account_ids()
    lane = lax.broadcasted_iota(I32, (ACCOUNTS, LANES), 1).astype(F32)
    account_f = account.astype(F32)

    def owner_of(slot):
        return jnp.bitwise_xor(slot, flip)

    def find_last(slot, carry):
        kept = jnp.where((home == owner_of(slot)) & (flag == 1), account_f, -1.0).astype(BF16)
        latest = jnp.full((ACCOUNTS, LANES), -1.0, BF16)
        for tile in range(tiles):
            latest = jnp.where(kept[tile : tile + 1] == ids, small(tile), latest)
        latest = latest.astype(F32)
        place = jnp.where(latest >= 0.0, latest * LANES + lane, -1.0)
        last_ref[pl.ds(slot, 1), :] = jnp.max(place.T, axis=0, keepdims=True)
        return carry

    lax.fori_loop(0, slots, find_last, 0, unroll=min(slots, 8))

    def look_up(slot, least):
        row = jnp.broadcast_to(last_ref[pl.ds(slot, 1), :], (tiles, LANES))
        found = jnp.take_along_axis(row, account, axis=1)
        return jnp.where(home == owner_of(slot), found, least)

    least = jnp.full((tiles, LANES), -1.0, F32)
    least = lax.fori_loop(0, slots, look_up, least, unroll=min(slots, 8))
    live = row_positions(tiles).astype(F32) >= least
    weight = jnp.where(flag == 1, 65.0, 1.0).astype(BF16)
    copies[3].wait()
    high, low = split_two(x_ref[...])
    parts_ref[:, 0:features] = high
    parts_ref[:, features : 2 * features] = low

    def one_group(number, out_ref, base):
        kept = [
            jnp.where(live & (home == owner_of(base + number * group + i)), account_f, -1.0).astype(BF16)
            for i in range(group)
        ]
        total = jnp.zeros((group * ACCOUNTS, 2 * features), F32)
        counts = [jnp.zeros((ACCOUNTS, LANES), BF16) for _ in range(group)]
        for begin in range(0, events, chunk):
            blocks = []
            for i in range(group):
                pieces = []
                for tile in range(begin // LANES, (begin + chunk) // LANES):
                    mask = kept[i][tile : tile + 1] == ids
                    share = jnp.broadcast_to(weight[tile : tile + 1], mask.shape)
                    counts[i] = counts[i] + jnp.where(mask, share, small(0.0))
                    pieces.append(jnp.where(mask, small(1.0), small(0.0)))
                blocks.append(jnp.concatenate(pieces, axis=1))
            total = total + jnp.dot(
                jnp.concatenate(blocks, axis=0),
                parts_ref[begin : begin + chunk, :],
                preferred_element_type=F32,
            )
        sums = total[:, 0:features] + total[:, features : 2 * features]
        for i in range(group):
            place = number * group + i
            out_ref[place, 0:features, :] = sums[i * ACCOUNTS : (i + 1) * ACCOUNTS].T
            count = counts[i].astype(F32)
            count = jnp.where(count >= 64.0, count + (8192.0 - 64.0), count)
            tally = jnp.sum(count.T, axis=0, keepdims=True)
            marked = jnp.where(tally >= 8192.0, 1.0, 0.0)
            spot = lax.broadcasted_iota(I32, (rows - features, LANES), 0)
            out_ref[place, features:rows, :] = jnp.where(
                spot == 0, tally - 8192.0 * marked, jnp.where(spot == 1, marked, 0.0)
            )

    def both(number, carry):
        one_group(number, sent_ref, half)
        one_group(number, kept_ref, 0)
        return carry

    lax.fori_loop(0, half // group, both, 0, unroll=min(half // group, 2))


def turn(row):
    return jnp.broadcast_to(row, (LANES, LANES)).T


def parts_kernel(x_ref, parts_ref):
    events, features = x_ref.shape
    rows = parts_ref.shape[0]
    for first in range(0, events, LANES):
        span = slice(first, first + LANES)
        high, low = split_two(x_ref[span, :].T)
        parts_ref[0:features, span] = high
        parts_ref[features : 2 * features, span] = low
    extra = lax.broadcasted_iota(I32, (rows - 2 * features, events), 0)
    parts_ref[2 * features : rows, :] = jnp.where(extra == 0, 1.0, 0.0).astype(BF16)


def stats_kernel(
    home_ref, account_ref, flag_ref, column_ref, sid_ref, key_ref, start_ref, *, owners
):
    tiles = home_ref.shape[0]
    events = tiles * LANES
    per = 4 if tiles % 8 == 0 else tiles
    home, account, flag = home_ref[...], account_ref[...], flag_ref[...]
    account_f = account.astype(F32)
    user = home * ACCOUNTS + account
    user_f = user.astype(F32)
    flagged = jnp.where(flag == 1, user_f, -1.0)
    row_id = lax.broadcasted_iota(I32, (LANES, LANES), 0)
    reaches = row_id <= lax.broadcasted_iota(I32, (LANES, LANES), 1)
    spot = row_id.astype(F32)
    lane = lax.broadcasted_iota(I32, (ACCOUNTS, LANES), 1).astype(F32)
    ids = account_ids()
    upper = lax.broadcasted_iota(I32, (8, LANES), 0) >= 4

    def before_block(owner, least):
        mine = home == owner
        kept = jnp.where(mine & (flag == 1), account_f, -1.0).astype(BF16)
        latest = jnp.full((ACCOUNTS, LANES), -1.0, BF16)
        rows = [jnp.full((1, LANES), -1.0, F32)]
        for tile in range(tiles - per):
            latest = jnp.where(kept[tile : tile + 1] == ids, small(tile), latest)
            if (tile + 1) % per == 0:
                place = latest.astype(F32)
                place = jnp.where(place >= 0.0, place * LANES + lane, -1.0)
                rows.append(jnp.max(place.T, axis=0, keepdims=True))
        if per == tiles:
            wide = jnp.broadcast_to(rows[0], (tiles, LANES))
        else:
            wide = jnp.concatenate(
                [jnp.where(upper, rows[i + 1], rows[i]) for i in range(0, len(rows), 2)], axis=0
            )
        return jnp.where(mine, jnp.take_along_axis(wide, account, axis=1), least)

    base = jnp.full((tiles, LANES), -1.0, F32)
    base = lax.fori_loop(0, owners, before_block, base, unroll=min(owners, 8))

    for first in range(0, tiles, per):
        columns = [turn(flagged[tile : tile + 1]) for tile in range(first, first + per)]
        for tile in range(first, first + per):
            line = user_f[tile : tile + 1]
            latest = jnp.full((LANES, LANES), -1.0, F32)
            for other in range(first, tile + 1):
                mask = columns[other - first] == line
                if other == tile:
                    mask = mask & reaches
                latest = jnp.where(mask, float(other), latest)
            place = jnp.where(latest < 0.0, -1.0, latest * LANES + spot)
            start_ref[tile : tile + 1, :] = jnp.maximum(
                base[tile : tile + 1], jnp.max(place, axis=0, keepdims=True)
            )
    start = start_ref[...]
    key_ref[...] = jnp.where(start < 0.0, user, -1)
    sid = jnp.where(start < 0.0, user_f + float(events), start)
    sid_ref[...] = sid
    for tile in range(tiles):
        column_ref[tile * LANES : (tile + 1) * LANES, :] = turn(sid[tile : tile + 1])


def local_kernel(parts_ref, column_ref, sid_ref, out_ref, mask_ref, *, first, chunk):
    features = out_ref.shape[0] - EXTRA
    reaches = lax.broadcasted_iota(I32, (LANES, LANES), 0) <= lax.broadcasted_iota(
        I32, (LANES, LANES), 1
    )
    sid = sid_ref[...]
    for begin in range(first, first + out_ref.shape[1], chunk):
        slot = (begin // chunk) % 2
        depth = begin + chunk
        lines = [sid[t : t + 1] for t in range(begin // LANES, depth // LANES)]
        for c in range(0, depth, LANES):
            column = column_ref[c : c + LANES, :]
            for i, line in enumerate(lines):
                r = begin + i * LANES
                if c > r:
                    block = jnp.zeros((LANES, LANES), BF16)
                else:
                    mask = column == line
                    if c == r:
                        mask = mask & reaches
                    block = jnp.where(mask, 1.0, 0.0).astype(BF16)
                mask_ref[slot, c : c + LANES, i * LANES : (i + 1) * LANES] = block
        total = jnp.dot(
            parts_ref[:, 0:depth], mask_ref[slot, 0:depth, :], preferred_element_type=F32
        )
        span = slice(begin - first, begin - first + chunk)
        out_ref[0:features, span] = total[0:features] + total[features : 2 * features]
        out_ref[features:, span] = total[2 * features : 2 * features + EXTRA]


def gather_states(flip, first, key, state_ref, table_ref, chunk, finish):
    slots = state_ref.shape[0]
    events = key.shape[0] * LANES
    rows, features = table_ref.shape[0], state_ref.shape[1] - EXTRA
    group = min(8, slots)
    ids = account_ids()

    def fill(slot, carry):
        high, low = split_two(state_ref[slot, 0:features, :])
        span = pl.ds(pl.multiple_of(slot * ACCOUNTS, ACCOUNTS), ACCOUNTS)
        table_ref[0:features, span] = high
        table_ref[features : 2 * features, span] = low
        count = state_ref[slot, features : features + 1, :].astype(I32)
        digit = lax.broadcasted_iota(I32, (rows - 2 * features, LANES), 0)
        extra = jnp.where(
            digit == 0,
            lax.shift_right_logical(count, 16),
            jnp.where(
                digit == 1,
                lax.shift_right_logical(count, 8) & 255,
                jnp.where(digit == 2, count & 255, 0),
            ),
        )
        table_ref[2 * features : rows, span] = extra.astype(F32).astype(BF16)
        return carry

    lax.fori_loop(0, slots, fill, 0, unroll=min(slots, 8))
    account_f = (key & (ACCOUNTS - 1)).astype(F32)
    home = lax.shift_right_arithmetic(key, ACCOUNTS.bit_length() - 1)

    for begin in range(0, events, chunk):

        def part(step, total):
            lines = []
            for i in range(group):
                owner = jnp.bitwise_xor(first + step * group + i, flip)
                mine = jnp.where(home == owner, account_f, -1.0).astype(BF16)
                blocks = [
                    jnp.where(mine[tile : tile + 1] == ids, small(1.0), small(0.0))
                    for tile in range(begin // LANES, (begin + chunk) // LANES)
                ]
                lines.append(jnp.concatenate(blocks, axis=1))
            place = pl.ds(pl.multiple_of(step * group * ACCOUNTS, LANES), group * ACCOUNTS)
            found = jnp.dot(
                table_ref[:, place], jnp.concatenate(lines, axis=0), preferred_element_type=F32
            )
            return found if total is None else total + found

        if slots == group:
            total = part(0, None)
        else:
            total = lax.fori_loop(0, slots // group, part, jnp.zeros((rows, chunk), F32))
        more = total[2 * features : 2 * features + 3]
        count = more[0:1] * 65536.0 + more[1:2] * 256.0 + more[2:3]
        finish(begin, total[0:features] + total[features : 2 * features], count)


def gather_kernel(flip_ref, key_ref, state_ref, *refs, starts, chunk, first):
    local_refs, out_ref, table_ref = refs[: len(starts)], refs[-2], refs[-1]
    features = state_ref.shape[1] - EXTRA

    def finish(begin, sums, count):
        piece = max(i for i in range(len(starts)) if starts[i] <= begin)
        local_ref = local_refs[piece]
        span = slice(begin - starts[piece], begin - starts[piece] + chunk)
        out_ref[0:features, begin : begin + chunk] = local_ref[0:features, span] + sums
        out_ref[features : features + 1, begin : begin + chunk] = (
            local_ref[features : features + 1, span] + count
        )

    gather_states(flip_ref[0], first, key_ref[...], state_ref, table_ref, chunk, finish)


def final_kernel(
    flip_ref, key_ref, state_ref, sums_ref, out_ref, table_ref, stage_ref, sems, *, chunk, first
):
    features = state_ref.shape[1] - EXTRA
    copies = []

    def finish(begin, sums, count):
        span = slice(begin, begin + chunk)
        sums = sums_ref[0:features, span] + sums
        count = sums_ref[features : features + 1, span] + count
        stage_ref[span, :] = (sums * (1.0 / count)).T
        rows = pl.ds(begin, chunk)
        copy = pltpu.make_async_copy(
            stage_ref.at[rows, :], out_ref.at[rows, :], sems.at[begin // chunk]
        )
        copy.start()
        copies.append(copy)

    gather_states(flip_ref[0], first, key_ref[...], state_ref, table_ref, chunk, finish)
    for copy in copies:
        copy.wait()


VMEM = pl.BlockSpec(memory_space=pltpu.VMEM)
SMEM = pl.BlockSpec(memory_space=pltpu.SMEM)
HBM = pl.BlockSpec(memory_space=pltpu.HBM)
PARAMS = pltpu.CompilerParams(vmem_limit_bytes=28 * 1024 * 1024)


def closing_states(flip, home, account, flags, features, owners):
    events, width = features.shape
    tiles = events // LANES
    home, account, flags, features = [
        pltpu.with_memory_space_constraint(v, pltpu.HBM) for v in (home, account, flags, features)
    ]
    shape = jax.ShapeDtypeStruct((owners // 2, width + EXTRA, LANES), F32)
    return pl.pallas_call(
        closing_kernel,
        out_shape=(shape, shape),
        in_specs=[SMEM, HBM, HBM, HBM, HBM],
        out_specs=(VMEM, VMEM),
        scratch_shapes=[pltpu.VMEM((tiles, LANES), I32)] * 3
        + [
            pltpu.VMEM((events, width), F32),
            pltpu.VMEM((events, 2 * width), BF16),
            pltpu.VMEM((max(8, owners), LANES), F32),
            pltpu.SemaphoreType.DMA((4,)),
        ],
        compiler_params=PARAMS,
        name="closing",
    )(flip, home, account, flags, features)


def feature_parts(features):
    events, width = features.shape
    return pl.pallas_call(
        parts_kernel,
        out_shape=jax.ShapeDtypeStruct((2 * width + 16, events), BF16),
        in_specs=[VMEM],
        out_specs=VMEM,
        compiler_params=PARAMS,
        name="parts",
    )(features)


def event_stats(home, account, flags, owners):
    tiles = home.shape[0]
    return pl.pallas_call(
        functools.partial(stats_kernel, owners=owners),
        out_shape=(
            jax.ShapeDtypeStruct((tiles * LANES, LANES), F32),
            jax.ShapeDtypeStruct((tiles, LANES), F32),
            jax.ShapeDtypeStruct((tiles, LANES), I32),
        ),
        in_specs=[VMEM, VMEM, VMEM],
        out_specs=(VMEM, VMEM, VMEM),
        scratch_shapes=[pltpu.VMEM((tiles, LANES), F32)],
        compiler_params=PARAMS,
        name="stats",
    )(home, account, flags)


def local_sums(parts, column, sid, first, length, width):
    chunk = min(512, length)
    return pl.pallas_call(
        functools.partial(local_kernel, first=first, chunk=chunk),
        out_shape=jax.ShapeDtypeStruct((width + EXTRA, length), F32),
        in_specs=[VMEM, VMEM, VMEM],
        out_specs=VMEM,
        scratch_shapes=[pltpu.VMEM((2, first + length, chunk), BF16)],
        compiler_params=PARAMS,
        name="local",
    )(parts, column, sid)


def first_gather(flip, key, state, pieces, starts, events, width):
    chunk = min(512, events)
    return pl.pallas_call(
        functools.partial(gather_kernel, starts=starts, chunk=chunk, first=0),
        out_shape=jax.ShapeDtypeStruct((width + EXTRA, events), F32),
        in_specs=[SMEM, VMEM, VMEM] + [VMEM] * len(pieces),
        out_specs=VMEM,
        scratch_shapes=[pltpu.VMEM((2 * width + 16, state.shape[0] * ACCOUNTS), BF16)],
        compiler_params=PARAMS,
        name="gather",
    )(flip, key, state, *pieces)


def final_means(flip, key, state, sums, events, width, first):
    chunk = min(512, events)
    return pl.pallas_call(
        functools.partial(final_kernel, chunk=chunk, first=first),
        out_shape=jax.ShapeDtypeStruct((events, width), F32),
        in_specs=[SMEM, VMEM, VMEM, VMEM],
        out_specs=HBM,
        scratch_shapes=[
            pltpu.VMEM((2 * width + 16, state.shape[0] * ACCOUNTS), BF16),
            pltpu.VMEM((events, width), F32),
            pltpu.SemaphoreType.DMA((events // chunk,)),
        ],
        compiler_params=PARAMS,
        name="final",
    )(flip, key, state, sums)


def combine(earlier, later, mark):
    return later + (1.0 - later[:, mark : mark + 1, :]) * earlier


def pick(parts, bits):
    for place, bit in enumerate(bits):
        step = 1 << place
        parts = [jnp.where(bit, parts[i ^ step], parts[i]) for i in range(len(parts))]
    return parts


def levels_of(devices, owners):
    left, levels = min(devices, owners).bit_length() - 1, []
    for want in LEVELS:
        if left > 0:
            levels.append(min(want, left))
            left -= levels[-1]
    return levels


def scan_states(kept, sent, me, devices, width, levels):
    mark = width + 1
    state = None
    steps = devices.bit_length() - 1

    def swap(value, mask):
        return lax.ppermute(value, AXES, [(i, i ^ mask) for i in range(devices)])

    def bit(step):
        return ((me >> step) & 1) == 1

    saved, done = [], 0
    for level in levels:
        if done == 0:
            parts = [kept, sent]
        else:
            part = state.shape[0] >> level
            parts = [state[i * part : (i + 1) * part] for i in range(1 << level)]
        got = [parts[0]]
        for other in range(1, 1 << level):
            piece = parts[other]
            got.append(swap(piece, other << done))
        bits = [bit(done + i) for i in range(level)]
        ordered = pick(got, bits)
        saved.append((done, bits, ordered))
        state = ordered[0]
        for later in ordered[1:]:
            state = combine(state, later, mark)
        done += level
    before = jnp.zeros_like(state)
    while done < steps:
        level = min(2, steps - done)
        got = [state]
        for other in range(1, 1 << level):
            got.append(swap(state, other << done))
        bits = [bit(done + i) for i in range(level)]
        ordered = pick(got, bits)
        earlier = [jnp.zeros_like(state), ordered[0]]
        for later in ordered[1:-1]:
            earlier.append(combine(earlier[-1], later, mark))
        before = combine(pick(earlier, bits)[0], before, mark)
        done += level
        if done < steps:
            state = combine(earlier[-1], ordered[-1], mark)
    for done, bits, ordered in reversed(saved):
        prefixes = [before]
        for earlier in ordered[:-1]:
            prefixes.append(combine(prefixes[-1], earlier, mark))
        mine = pick(prefixes, bits)
        got = [mine[0]]
        for other in range(1, len(mine)):
            got.append(swap(mine[other], other << done))
        if done == 0:
            return got
        before = jnp.concatenate(got, axis=0)


def flip_of(me, levels, owners):
    flip, done, top = jnp.zeros((), I32), 0, owners.bit_length() - 1
    for level in levels:
        top -= level
        flip = flip | (((me >> done) & ((1 << level) - 1)) << top)
        done += level
    return flip.reshape(1)


def body(features, home, account, flags):
    owners = lax.axis_size("users")
    devices = lax.axis_size("tm") * owners
    events, width = features.shape
    tiles = events // LANES
    me = lax.axis_index("tm") * owners + lax.axis_index("users")
    levels = levels_of(devices, owners)
    flip = flip_of(me, levels, owners)
    home2 = home.reshape(tiles, LANES)
    account2 = account.reshape(tiles, LANES)
    flags2 = flags.reshape(tiles, LANES)
    half = owners // 2
    kept, sent = closing_states(flip, home2, account2, flags2, features, owners)
    column, sid, key = event_stats(home2, account2, flags2, owners)
    parts = feature_parts(features)
    starts = [events * i // 8 for i in STARTS]
    pieces = []
    for i, first in enumerate(starts):
        length = (starts + [events])[i + 1] - first
        pieces.append(local_sums(parts, column, sid, first, length, width))
    mine, theirs = scan_states(kept, sent, me, devices, width, levels)
    sums = first_gather(flip, key, mine, pieces, starts, events, width)
    return final_means(flip, key, theirs, sums, events, width, half)


def solution(mesh):
    return jax.shard_map(
        body,
        mesh=mesh,
        in_specs=(P(AXES, None), P(AXES, None), P(AXES), P(AXES)),
        out_specs=P(AXES, None),
        check_vma=False,
    )
```

```python
import functools

import jax
import jax.numpy as jnp
from jax import lax
from jax.experimental import pallas as pl
from jax.experimental.pallas import tpu as pltpu
from jax.sharding import PartitionSpec as P


ACCOUNTS = 128
LANES = 128
EXTRA = 8
LEVELS = (1, 2)
STARTS = (0, 3, 5, 7)
AXES = ("tm", "users")
F32, BF16, I32 = jnp.float32, jnp.bfloat16, jnp.int32


def split_two(x):
    high = x.astype(BF16)
    return high, (x - high.astype(F32)).astype(BF16)


def account_ids():
    return lax.broadcasted_iota(I32, (ACCOUNTS, LANES), 0).astype(F32).astype(BF16)


def row_positions(tiles):
    shape = (tiles, LANES)
    return lax.broadcasted_iota(I32, shape, 0) * LANES + lax.broadcasted_iota(I32, shape, 1)


def small(value):
    return jnp.asarray(value, BF16)


def closing_kernel(
    flip_ref,
    home_hbm,
    account_hbm,
    flag_hbm,
    x_hbm,
    kept_ref,
    sent_ref,
    home_ref,
    account_ref,
    flag_ref,
    x_ref,
    parts_ref,
    last_ref,
    sems,
):
    pairs = (
        (home_hbm, home_ref),
        (account_hbm, account_ref),
        (flag_hbm, flag_ref),
        (x_hbm, x_ref),
    )
    copies = [pltpu.make_async_copy(a, b, sems.at[i]) for i, (a, b) in enumerate(pairs)]
    for copy in copies:
        copy.start()
    for copy in copies[:3]:
        copy.wait()
    home, account, flag = home_ref[...], account_ref[...], flag_ref[...]
    flip = flip_ref[0]
    tiles = home.shape[0]
    half, rows = kept_ref.shape[0], kept_ref.shape[1]
    slots = 2 * half
    events, features = x_ref.shape
    chunk = min(512, events)
    group = 2 if half % 2 == 0 else 1
    ids = account_ids()
    lane = lax.broadcasted_iota(I32, (ACCOUNTS, LANES), 1).astype(F32)
    account_f = account.astype(F32)

    def owner_of(slot):
        return jnp.bitwise_xor(slot, flip)

    def find_last(slot, carry):
        kept = jnp.where((home == owner_of(slot)) & (flag == 1), account_f, -1.0).astype(BF16)
        latest = jnp.full((ACCOUNTS, LANES), -1.0, BF16)
        for tile in range(tiles):
            latest = jnp.where(kept[tile : tile + 1] == ids, small(tile), latest)
        latest = latest.astype(F32)
        place = jnp.where(latest >= 0.0, latest * LANES + lane, -1.0)
        last_ref[pl.ds(slot, 1), :] = jnp.max(place.T, axis=0, keepdims=True)
        return carry

    lax.fori_loop(0, slots, find_last, 0, unroll=min(slots, 8))

    def look_up(slot, least):
        row = jnp.broadcast_to(last_ref[pl.ds(slot, 1), :], (tiles, LANES))
        found = jnp.take_along_axis(row, account, axis=1)
        return jnp.where(home == owner_of(slot), found, least)

    least = jnp.full((tiles, LANES), -1.0, F32)
    least = lax.fori_loop(0, slots, look_up, least, unroll=min(slots, 8))
    live = row_positions(tiles).astype(F32) >= least
    weight = jnp.where(flag == 1, 65.0, 1.0).astype(BF16)
    copies[3].wait()
    high, low = split_two(x_ref[...])
    parts_ref[:, 0:features] = high
    parts_ref[:, features : 2 * features] = low

    def one_group(number, out_ref, base):
        kept = [
            jnp.where(live & (home == owner_of(base + number * group + i)), account_f, -1.0).astype(BF16)
            for i in range(group)
        ]
        total = jnp.zeros((group * ACCOUNTS, 2 * features), F32)
        counts = [jnp.zeros((ACCOUNTS, LANES), BF16) for _ in range(group)]
        for begin in range(0, events, chunk):
            blocks = []
            for i in range(group):
                pieces = []
                for tile in range(begin // LANES, (begin + chunk) // LANES):
                    mask = kept[i][tile : tile + 1] == ids
                    share = jnp.broadcast_to(weight[tile : tile + 1], mask.shape)
                    counts[i] = counts[i] + jnp.where(mask, share, small(0.0))
                    pieces.append(jnp.where(mask, small(1.0), small(0.0)))
                blocks.append(jnp.concatenate(pieces, axis=1))
            total = total + jnp.dot(
                jnp.concatenate(blocks, axis=0),
                parts_ref[begin : begin + chunk, :],
                preferred_element_type=F32,
            )
        sums = total[:, 0:features] + total[:, features : 2 * features]
        for i in range(group):
            place = number * group + i
            out_ref[place, 0:features, :] = sums[i * ACCOUNTS : (i + 1) * ACCOUNTS].T
            count = counts[i].astype(F32)
            count = jnp.where(count >= 64.0, count + (8192.0 - 64.0), count)
            tally = jnp.sum(count.T, axis=0, keepdims=True)
            marked = jnp.where(tally >= 8192.0, 1.0, 0.0)
            spot = lax.broadcasted_iota(I32, (rows - features, LANES), 0)
            out_ref[place, features:rows, :] = jnp.where(
                spot == 0, tally - 8192.0 * marked, jnp.where(spot == 1, marked, 0.0)
            )

    def both(number, carry):
        one_group(number, sent_ref, half)
        one_group(number, kept_ref, 0)
        return carry

    lax.fori_loop(0, half // group, both, 0, unroll=min(half // group, 2))


def turn(row):
    return jnp.broadcast_to(row, (LANES, LANES)).T


def parts_kernel(x_ref, parts_ref):
    events, features = x_ref.shape
    rows = parts_ref.shape[0]
    for first in range(0, events, LANES):
        span = slice(first, first + LANES)
        high, low = split_two(x_ref[span, :].T)
        parts_ref[0:features, span] = high
        parts_ref[features : 2 * features, span] = low
    extra = lax.broadcasted_iota(I32, (rows - 2 * features, events), 0)
    parts_ref[2 * features : rows, :] = jnp.where(extra == 0, 1.0, 0.0).astype(BF16)


def stats_kernel(
    home_ref, account_ref, flag_ref, column_ref, sid_ref, key_ref, start_ref, *, owners
):
    tiles = home_ref.shape[0]
    events = tiles * LANES
    per = 4 if tiles % 8 == 0 else tiles
    home, account, flag = home_ref[...], account_ref[...], flag_ref[...]
    account_f = account.astype(F32)
    user = home * ACCOUNTS + account
    user_f = user.astype(F32)
    flagged = jnp.where(flag == 1, user_f, -1.0)
    row_id = lax.broadcasted_iota(I32, (LANES, LANES), 0)
    reaches = row_id <= lax.broadcasted_iota(I32, (LANES, LANES), 1)
    spot = row_id.astype(F32)
    lane = lax.broadcasted_iota(I32, (ACCOUNTS, LANES), 1).astype(F32)
    ids = account_ids()
    upper = lax.broadcasted_iota(I32, (8, LANES), 0) >= 4

    def before_block(owner, least):
        mine = home == owner
        kept = jnp.where(mine & (flag == 1), account_f, -1.0).astype(BF16)
        latest = jnp.full((ACCOUNTS, LANES), -1.0, BF16)
        rows = [jnp.full((1, LANES), -1.0, F32)]
        for tile in range(tiles - per):
            latest = jnp.where(kept[tile : tile + 1] == ids, small(tile), latest)
            if (tile + 1) % per == 0:
                place = latest.astype(F32)
                place = jnp.where(place >= 0.0, place * LANES + lane, -1.0)
                rows.append(jnp.max(place.T, axis=0, keepdims=True))
        if per == tiles:
            wide = jnp.broadcast_to(rows[0], (tiles, LANES))
        else:
            wide = jnp.concatenate(
                [jnp.where(upper, rows[i + 1], rows[i]) for i in range(0, len(rows), 2)], axis=0
            )
        return jnp.where(mine, jnp.take_along_axis(wide, account, axis=1), least)

    base = jnp.full((tiles, LANES), -1.0, F32)
    base = lax.fori_loop(0, owners, before_block, base, unroll=min(owners, 8))

    for first in range(0, tiles, per):
        columns = [turn(flagged[tile : tile + 1]) for tile in range(first, first + per)]
        for tile in range(first, first + per):
            line = user_f[tile : tile + 1]
            latest = jnp.full((LANES, LANES), -1.0, F32)
            for other in range(first, tile + 1):
                mask = columns[other - first] == line
                if other == tile:
                    mask = mask & reaches
                latest = jnp.where(mask, float(other), latest)
            place = jnp.where(latest < 0.0, -1.0, latest * LANES + spot)
            start_ref[tile : tile + 1, :] = jnp.maximum(
                base[tile : tile + 1], jnp.max(place, axis=0, keepdims=True)
            )
    start = start_ref[...]
    key_ref[...] = jnp.where(start < 0.0, user, -1)
    sid = jnp.where(start < 0.0, user_f + float(events), start)
    sid_ref[...] = sid
    for tile in range(tiles):
        column_ref[tile * LANES : (tile + 1) * LANES, :] = turn(sid[tile : tile + 1])


def local_kernel(parts_ref, column_ref, sid_ref, out_ref, mask_ref, *, first, chunk):
    features = out_ref.shape[0] - EXTRA
    reaches = lax.broadcasted_iota(I32, (LANES, LANES), 0) <= lax.broadcasted_iota(
        I32, (LANES, LANES), 1
    )
    sid = sid_ref[...]
    for begin in range(first, first + out_ref.shape[1], chunk):
        slot = (begin // chunk) % 2
        depth = begin + chunk
        lines = [sid[t : t + 1] for t in range(begin // LANES, depth // LANES)]
        for c in range(0, depth, LANES):
            column = column_ref[c : c + LANES, :]
            for i, line in enumerate(lines):
                r = begin + i * LANES
                if c > r:
                    block = jnp.zeros((LANES, LANES), BF16)
                else:
                    mask = column == line
                    if c == r:
                        mask = mask & reaches
                    block = jnp.where(mask, 1.0, 0.0).astype(BF16)
                mask_ref[slot, c : c + LANES, i * LANES : (i + 1) * LANES] = block
        total = jnp.dot(
            parts_ref[:, 0:depth], mask_ref[slot, 0:depth, :], preferred_element_type=F32
        )
        span = slice(begin - first, begin - first + chunk)
        out_ref[0:features, span] = total[0:features] + total[features : 2 * features]
        out_ref[features:, span] = total[2 * features : 2 * features + EXTRA]


def gather_states(flip, first, key, state_ref, table_ref, chunk, tail, finish):
    slots = state_ref.shape[0]
    events = key.shape[0] * LANES
    rows, features = table_ref.shape[0], state_ref.shape[1] - EXTRA
    group = min(8, slots)
    ids = account_ids()

    def fill(slot, carry):
        high, low = split_two(state_ref[slot, 0:features, :])
        span = pl.ds(pl.multiple_of(slot * ACCOUNTS, ACCOUNTS), ACCOUNTS)
        table_ref[0:features, span] = high
        table_ref[features : 2 * features, span] = low
        count = state_ref[slot, features : features + 1, :].astype(I32)
        digit = lax.broadcasted_iota(I32, (rows - 2 * features, LANES), 0)
        extra = jnp.where(
            digit == 0,
            lax.shift_right_logical(count, 16),
            jnp.where(
                digit == 1,
                lax.shift_right_logical(count, 8) & 255,
                jnp.where(digit == 2, count & 255, 0),
            ),
        )
        table_ref[2 * features : rows, span] = extra.astype(F32).astype(BF16)
        return carry

    lax.fori_loop(0, slots, fill, 0, unroll=min(slots, 8))
    account_f = (key & (ACCOUNTS - 1)).astype(F32)
    home = lax.shift_right_arithmetic(key, ACCOUNTS.bit_length() - 1)

    spans = [(begin, chunk) for begin in range(0, events, chunk)]
    if tail < chunk:
        begin = spans.pop()[0]
        spans += [(first, tail) for first in range(begin, events, tail)]
    for begin, chunk in spans:

        def part(step, total):
            lines = []
            for i in range(group):
                owner = jnp.bitwise_xor(first + step * group + i, flip)
                mine = jnp.where(home == owner, account_f, -1.0).astype(BF16)
                blocks = [
                    jnp.where(mine[tile : tile + 1] == ids, small(1.0), small(0.0))
                    for tile in range(begin // LANES, (begin + chunk) // LANES)
                ]
                lines.append(jnp.concatenate(blocks, axis=1))
            place = pl.ds(pl.multiple_of(step * group * ACCOUNTS, LANES), group * ACCOUNTS)
            found = jnp.dot(
                table_ref[:, place], jnp.concatenate(lines, axis=0), preferred_element_type=F32
            )
            return found if total is None else total + found

        if slots == group:
            total = part(0, None)
        else:
            total = lax.fori_loop(0, slots // group, part, jnp.zeros((rows, chunk), F32))
        more = total[2 * features : 2 * features + 3]
        count = more[0:1] * 65536.0 + more[1:2] * 256.0 + more[2:3]
        finish(begin, chunk, total[0:features] + total[features : 2 * features], count)


def gather_kernel(flip_ref, key_ref, state_ref, *refs, starts, chunk, first):
    local_refs, out_ref, table_ref = refs[: len(starts)], refs[-2], refs[-1]
    features = state_ref.shape[1] - EXTRA

    def finish(begin, chunk, sums, count):
        piece = max(i for i in range(len(starts)) if starts[i] <= begin)
        local_ref = local_refs[piece]
        span = slice(begin - starts[piece], begin - starts[piece] + chunk)
        out_ref[0:features, begin : begin + chunk] = local_ref[0:features, span] + sums
        out_ref[features : features + 1, begin : begin + chunk] = (
            local_ref[features : features + 1, span] + count
        )

    gather_states(flip_ref[0], first, key_ref[...], state_ref, table_ref, chunk, chunk, finish)


def final_kernel(
    flip_ref, key_ref, state_ref, sums_ref, out_ref, table_ref, stage_ref, sems, *, chunk, tail, first
):
    features = state_ref.shape[1] - EXTRA
    copies = []

    def finish(begin, chunk, sums, count):
        span = slice(begin, begin + chunk)
        sums = sums_ref[0:features, span] + sums
        count = sums_ref[features : features + 1, span] + count
        stage_ref[span, :] = (sums * (1.0 / count)).T
        rows = pl.ds(begin, chunk)
        copy = pltpu.make_async_copy(
            stage_ref.at[rows, :], out_ref.at[rows, :], sems.at[len(copies)]
        )
        copy.start()
        copies.append(copy)

    gather_states(flip_ref[0], first, key_ref[...], state_ref, table_ref, chunk, tail, finish)
    for copy in copies:
        copy.wait()


VMEM = pl.BlockSpec(memory_space=pltpu.VMEM)
SMEM = pl.BlockSpec(memory_space=pltpu.SMEM)
HBM = pl.BlockSpec(memory_space=pltpu.HBM)
PARAMS = pltpu.CompilerParams(vmem_limit_bytes=28 * 1024 * 1024)


def closing_states(flip, home, account, flags, features, owners):
    events, width = features.shape
    tiles = events // LANES
    home, account, flags, features = [
        pltpu.with_memory_space_constraint(v, pltpu.HBM) for v in (home, account, flags, features)
    ]
    shape = jax.ShapeDtypeStruct((owners // 2, width + EXTRA, LANES), F32)
    return pl.pallas_call(
        closing_kernel,
        out_shape=(shape, shape),
        in_specs=[SMEM, HBM, HBM, HBM, HBM],
        out_specs=(VMEM, VMEM),
        scratch_shapes=[pltpu.VMEM((tiles, LANES), I32)] * 3
        + [
            pltpu.VMEM((events, width), F32),
            pltpu.VMEM((events, 2 * width), BF16),
            pltpu.VMEM((max(8, owners), LANES), F32),
            pltpu.SemaphoreType.DMA((4,)),
        ],
        compiler_params=PARAMS,
        name="closing",
    )(flip, home, account, flags, features)


def feature_parts(features):
    events, width = features.shape
    return pl.pallas_call(
        parts_kernel,
        out_shape=jax.ShapeDtypeStruct((2 * width + 16, events), BF16),
        in_specs=[VMEM],
        out_specs=VMEM,
        compiler_params=PARAMS,
        name="parts",
    )(features)


def event_stats(home, account, flags, owners):
    tiles = home.shape[0]
    return pl.pallas_call(
        functools.partial(stats_kernel, owners=owners),
        out_shape=(
            jax.ShapeDtypeStruct((tiles * LANES, LANES), F32),
            jax.ShapeDtypeStruct((tiles, LANES), F32),
            jax.ShapeDtypeStruct((tiles, LANES), I32),
        ),
        in_specs=[VMEM, VMEM, VMEM],
        out_specs=(VMEM, VMEM, VMEM),
        scratch_shapes=[pltpu.VMEM((tiles, LANES), F32)],
        compiler_params=PARAMS,
        name="stats",
    )(home, account, flags)


def local_sums(parts, column, sid, first, length, width):
    chunk = min(512, length)
    return pl.pallas_call(
        functools.partial(local_kernel, first=first, chunk=chunk),
        out_shape=jax.ShapeDtypeStruct((width + EXTRA, length), F32),
        in_specs=[VMEM, VMEM, VMEM],
        out_specs=VMEM,
        scratch_shapes=[pltpu.VMEM((2, first + length, chunk), BF16)],
        compiler_params=PARAMS,
        name="local",
    )(parts, column, sid)


def first_gather(flip, key, state, pieces, starts, events, width):
    chunk = min(512, events)
    return pl.pallas_call(
        functools.partial(gather_kernel, starts=starts, chunk=chunk, first=0),
        out_shape=jax.ShapeDtypeStruct((width + EXTRA, events), F32),
        in_specs=[SMEM, VMEM, VMEM] + [VMEM] * len(pieces),
        out_specs=VMEM,
        scratch_shapes=[pltpu.VMEM((2 * width + 16, state.shape[0] * ACCOUNTS), BF16)],
        compiler_params=PARAMS,
        name="gather",
    )(flip, key, state, *pieces)


def final_means(flip, key, state, sums, events, width, first):
    chunk = min(512, events)
    return pl.pallas_call(
        functools.partial(final_kernel, chunk=chunk, tail=min(256, chunk), first=first),
        out_shape=jax.ShapeDtypeStruct((events, width), F32),
        in_specs=[SMEM, VMEM, VMEM, VMEM],
        out_specs=HBM,
        scratch_shapes=[
            pltpu.VMEM((2 * width + 16, state.shape[0] * ACCOUNTS), BF16),
            pltpu.VMEM((events, width), F32),
            pltpu.SemaphoreType.DMA((events // chunk + 1,)),
        ],
        compiler_params=PARAMS,
        name="final",
    )(flip, key, state, sums)


def combine(earlier, later, mark):
    return later + (1.0 - later[:, mark : mark + 1, :]) * earlier


def pick(parts, bits):
    for place, bit in enumerate(bits):
        step = 1 << place
        parts = [jnp.where(bit, parts[i ^ step], parts[i]) for i in range(len(parts))]
    return parts


def levels_of(devices, owners):
    left, levels = min(devices, owners).bit_length() - 1, []
    for want in LEVELS:
        if left > 0:
            levels.append(min(want, left))
            left -= levels[-1]
    return levels


def scan_states(kept, sent, me, devices, width, levels):
    mark = width + 1
    state = None
    steps = devices.bit_length() - 1

    def swap(value, mask):
        return lax.ppermute(value, AXES, [(i, i ^ mask) for i in range(devices)])

    def bit(step):
        return ((me >> step) & 1) == 1

    saved, done = [], 0
    for level in levels:
        if done == 0:
            parts = [kept, sent]
        else:
            part = state.shape[0] >> level
            parts = [state[i * part : (i + 1) * part] for i in range(1 << level)]
        got = [parts[0]]
        for other in range(1, 1 << level):
            piece = parts[other]
            got.append(swap(piece, other << done))
        bits = [bit(done + i) for i in range(level)]
        ordered = pick(got, bits)
        inside = [jnp.zeros_like(ordered[0]), ordered[0]]
        for later in ordered[1:]:
            inside.append(combine(inside[-1], later, mark))
        state = inside.pop()
        saved.append((done, pick(inside, bits)))
        done += level
    before = jnp.zeros_like(state)
    while done < steps:
        level = min(2, steps - done)
        got = [state]
        for other in range(1, 1 << level):
            got.append(swap(state, other << done))
        bits = [bit(done + i) for i in range(level)]
        ordered = pick(got, bits)
        earlier = [jnp.zeros_like(state), ordered[0]]
        for later in ordered[1:-1]:
            earlier.append(combine(earlier[-1], later, mark))
        before = combine(pick(earlier, bits)[0], before, mark)
        done += level
        if done < steps:
            state = combine(earlier[-1], ordered[-1], mark)
    for done, inside in reversed(saved):
        got = [combine(before, inside[0], mark)]
        for other in range(1, len(inside)):
            ahead = combine(before, inside[other], mark)
            got.append(swap(ahead, other << done))
        if done == 0:
            return got
        before = jnp.concatenate(got, axis=0)


def flip_of(me, levels, owners):
    flip, done, top = jnp.zeros((), I32), 0, owners.bit_length() - 1
    for level in levels:
        top -= level
        flip = flip | (((me >> done) & ((1 << level) - 1)) << top)
        done += level
    return flip.reshape(1)


def body(features, home, account, flags):
    owners = lax.axis_size("users")
    devices = lax.axis_size("tm") * owners
    events, width = features.shape
    tiles = events // LANES
    me = lax.axis_index("tm") * owners + lax.axis_index("users")
    levels = levels_of(devices, owners)
    flip = flip_of(me, levels, owners)
    home2 = home.reshape(tiles, LANES)
    account2 = account.reshape(tiles, LANES)
    flags2 = flags.reshape(tiles, LANES)
    half = owners // 2
    kept, sent = closing_states(flip, home2, account2, flags2, features, owners)
    column, sid, key = event_stats(home2, account2, flags2, owners)
    parts = feature_parts(features)
    starts = [events * i // 8 for i in STARTS]
    pieces = []
    for i, first in enumerate(starts):
        length = (starts + [events])[i + 1] - first
        pieces.append(local_sums(parts, column, sid, first, length, width))
    mine, theirs = scan_states(kept, sent, me, devices, width, levels)
    sums = first_gather(flip, key, mine, pieces, starts, events, width)
    return final_means(flip, key, theirs, sums, events, width, half)


def solution(mesh):
    return jax.shard_map(
        body,
        mesh=mesh,
        in_specs=(P(AXES, None), P(AXES, None), P(AXES), P(AXES)),
        out_specs=P(AXES, None),
        check_vma=False,
    )
```
